8 devices in a mesh: part: 1 (over z), cp: 2 (over y), sp: 4 (over x, core).
Axes of the slice: x: 2, y: 2, z: 1, core: 2. Of those that a mesh axis runs over, the one named last changes fastest.
Arguments:
- hidden: bfloat16 [1, 3072, 3072], P('part', ('cp', 'sp'))
- valid_mask: int32 [1, 3072], P('part', ('cp', 'sp'))
- positions: int32 [1, 3072, 3], P('part', ('cp', 'sp'))
- cond_vec: float32 [1, 3072], P('part')
- w_mod: bfloat16 [2, 3072, 9216], replicated
- b_mod: bfloat16 [2, 9216], replicated
- w_in: bfloat16 [2, 3072, 21504], replicated
- b_in: bfloat16 [2, 21504], replicated
- q_gain: bfloat16 [2, 128], replicated
- k_gain: bfloat16 [2, 128], replicated
- w_out: bfloat16 [2, 15360, 3072], replicated
- b_out: bfloat16 [2, 3072], replicated
Outputs:
- output: bfloat16 [1, 3072, 3072], P('part', ('cp', 'sp'))
All inputs are finite; a program needn't handle non-finite values.
Results may differ from the reference program's by a relative error of at most 0.00695652.
Values are sent between devices in bfloat16 or wider.
A program may use at most 2.25 GiB of HBM per device.

```python
import math
import jax
import jax.numpy as jnp
from jax import lax

MODEL_DIM = 3072
HEADS = 24
HEAD_DIM = 128
MLP_DIM = 12288
TEXT_LEN = 256
SEQ_LEN = 3072
PAD_LEN = 64
LAYERS = 2
Q_BLOCK = 128

VIDEO_LEN = SEQ_LEN - TEXT_LEN - PAD_LEN
PROJ_DIM = 3 * MODEL_DIM + MLP_DIM
ROPE_SPLIT = (16, 56, 56)
THETA = 256.0
EPS = 1e-6
SCORE_GAIN = math.log(SEQ_LEN / 4.0) ** 0.25


def setup_inputs(seed: int = 0, part: int = 0) -> dict:
    part_keys = jax.random.split(jax.random.fold_in(jax.random.key(seed), part), 8)
    shared_keys = jax.random.split(jax.random.key(seed + 1), 8)
    video_rows = jax.random.normal(part_keys[0], (VIDEO_LEN, MODEL_DIM), jnp.float32)
    text_common = jax.random.normal(part_keys[1], (1, MODEL_DIM), jnp.float32)
    text_rows = text_common + 0.4 * jax.random.normal(part_keys[2], (TEXT_LEN, MODEL_DIM), jnp.float32)
    pad_rows = jax.random.normal(part_keys[3], (PAD_LEN, MODEL_DIM), jnp.float32)
    hidden = jnp.concatenate([video_rows, text_rows, pad_rows], axis=0)[None].astype(jnp.bfloat16)
    token_idx = jnp.arange(SEQ_LEN)
    text_valid = jax.random.randint(part_keys[4], (), TEXT_LEN // 4, 3 * TEXT_LEN // 4 + 1)
    valid_mask = (token_idx < VIDEO_LEN + text_valid).astype(jnp.int32)[None]
    grid_top = jnp.array([32, 80, 80], jnp.int32)
    drawn_pos = jax.random.randint(part_keys[5], (SEQ_LEN, 3), 0, grid_top)
    positions = jnp.where((token_idx < VIDEO_LEN)[:, None], drawn_pos, 0).astype(jnp.int32)[None]
    cond_vec = jax.random.normal(part_keys[6], (1, MODEL_DIM), jnp.float32)
    w_mod = (jax.random.normal(shared_keys[0], (LAYERS, MODEL_DIM, 3 * MODEL_DIM), jnp.float32) * MODEL_DIM ** -0.5).astype(jnp.bfloat16)
    b_mod = (0.5 * jax.random.normal(shared_keys[1], (LAYERS, 3 * MODEL_DIM), jnp.float32)).astype(jnp.bfloat16)
    w_in = (jax.random.normal(shared_keys[2], (LAYERS, MODEL_DIM, PROJ_DIM), jnp.float32) * MODEL_DIM ** -0.5).astype(jnp.bfloat16)
    b_in = (0.5 * jax.random.normal(shared_keys[3], (LAYERS, PROJ_DIM), jnp.float32)).astype(jnp.bfloat16)
    q_gain = (SCORE_GAIN * jax.random.uniform(shared_keys[4], (LAYERS, HEAD_DIM), jnp.float32, 0.75, 1.25)).astype(jnp.bfloat16)
    k_gain = (SCORE_GAIN * jax.random.uniform(shared_keys[5], (LAYERS, HEAD_DIM), jnp.float32, 0.75, 1.25)).astype(jnp.bfloat16)
    row_scale = jnp.concatenate([jnp.full((MODEL_DIM,), 2.0, jnp.float32), jnp.ones((MLP_DIM,), jnp.float32)])
    w_out = (jax.random.normal(shared_keys[6], (LAYERS, MODEL_DIM + MLP_DIM, MODEL_DIM), jnp.float32) * (MODEL_DIM + MLP_DIM) ** -0.5 * row_scale[None, :, None]).astype(jnp.bfloat16)
    b_out = (0.5 * jax.random.normal(shared_keys[7], (LAYERS, MODEL_DIM), jnp.float32)).astype(jnp.bfloat16)
    return dict(hidden=hidden, valid_mask=valid_mask, positions=positions, cond_vec=cond_vec, w_mod=w_mod, b_mod=b_mod, w_in=w_in, b_in=b_in, q_gain=q_gain, k_gain=k_gain, w_out=w_out, b_out=b_out)


def rope_tables(positions):
    pieces = []
    for axis_idx, axis_width in enumerate(ROPE_SPLIT):
        frequencies = THETA ** (-jnp.arange(0, axis_width, 2).astype(jnp.float32) / axis_width)
        pieces.append(positions[..., axis_idx:axis_idx + 1].astype(jnp.float32) * frequencies)
    angles = jnp.concatenate(pieces, axis=-1)
    return jnp.cos(angles), jnp.sin(angles)


def norm_rotate(heads, gain, cos_t, sin_t):
    values = heads.astype(jnp.float32)
    values = values * lax.rsqrt(jnp.mean(values * values, axis=-1, keepdims=True) + EPS) * gain.astype(jnp.float32)
    pairs = values.reshape(values.shape[:-1] + (values.shape[-1] // 2, 2))
    pair_lo = pairs[..., 0]
    pair_hi = pairs[..., 1]
    cos_b = cos_t[..., None, :]
    sin_b = sin_t[..., None, :]
    rotated = jnp.stack([pair_lo * cos_b - pair_hi * sin_b, pair_hi * cos_b + pair_lo * sin_b], axis=-1)
    return rotated.reshape(heads.shape).astype(jnp.bfloat16)


def attend_all(q_heads, k_heads, v_heads, key_ok):
    score_scale = HEAD_DIM ** -0.5

    def per_head(operands):
        q_one, k_one, v_one = operands

        def per_block(q_blk):
            scores = jnp.dot(q_blk, k_one.T, preferred_element_type=jnp.float32) * score_scale
            scores = jnp.where(key_ok[None, :], scores, -1e30)
            row_max = jnp.max(scores, axis=-1, keepdims=True)
            weights = jnp.exp(scores - row_max)
            numerator = jnp.dot(weights.astype(jnp.bfloat16), v_one, preferred_element_type=jnp.float32)
            denominator = jnp.sum(weights, axis=-1, keepdims=True)
            return (numerator / denominator).astype(jnp.bfloat16)

        q_blocks = q_one.reshape(SEQ_LEN // Q_BLOCK, Q_BLOCK, HEAD_DIM)
        return lax.map(per_block, q_blocks).reshape(SEQ_LEN, HEAD_DIM)

    head_outs = lax.map(per_head, (jnp.swapaxes(q_heads, 0, 1), jnp.swapaxes(k_heads, 0, 1), jnp.swapaxes(v_heads, 0, 1)))
    return jnp.swapaxes(head_outs, 0, 1).reshape(SEQ_LEN, MODEL_DIM)


def reference(hidden, valid_mask, positions, cond_vec, w_mod, b_mod, w_in, b_in, q_gain, k_gain, w_out, b_out):
    cos_t, sin_t = rope_tables(positions[0])
    key_ok = valid_mask[0] > 0
    silu_vec = jax.nn.silu(cond_vec).astype(jnp.bfloat16)
    head_shape = (SEQ_LEN, HEADS, HEAD_DIM)

    def one_layer(state, layer_params):
        mod_w, mod_b, in_w, in_b, gain_q, gain_k, out_w, out_b = layer_params
        mod_vals = jnp.dot(silu_vec, mod_w, preferred_element_type=jnp.float32) + mod_b.astype(jnp.float32)
        shift_vec = mod_vals[:, :MODEL_DIM]
        scale_vec = mod_vals[:, MODEL_DIM:2 * MODEL_DIM]
        gate_vec = mod_vals[:, 2 * MODEL_DIM:]
        state_f = state.astype(jnp.float32)
        centered = state_f - jnp.mean(state_f, axis=-1, keepdims=True)
        variance = jnp.mean(centered * centered, axis=-1, keepdims=True)
        modded = (centered * lax.rsqrt(variance + EPS) * (1.0 + scale_vec) + shift_vec).astype(jnp.bfloat16)
        projected = (jnp.dot(modded, in_w, preferred_element_type=jnp.float32) + in_b.astype(jnp.float32)).astype(jnp.bfloat16)
        q_heads = norm_rotate(projected[:, :MODEL_DIM].reshape(head_shape), gain_q, cos_t, sin_t)
        k_heads = norm_rotate(projected[:, MODEL_DIM:2 * MODEL_DIM].reshape(head_shape), gain_k, cos_t, sin_t)
        v_heads = projected[:, 2 * MODEL_DIM:3 * MODEL_DIM].reshape(head_shape)
        attended = attend_all(q_heads, k_heads, v_heads, key_ok)
        mlp_act = jax.nn.gelu(projected[:, 3 * MODEL_DIM:].astype(jnp.float32), approximate=True).astype(jnp.bfloat16)
        joined = jnp.concatenate([attended, mlp_act], axis=-1)
        branch_out = jnp.dot(joined, out_w, preferred_element_type=jnp.float32) + out_b.astype(jnp.float32)
        new_state = (state_f + gate_vec * branch_out).astype(jnp.bfloat16)
        return new_state, None

    final_state, _ = lax.scan(one_layer, hidden[0], (w_mod, b_mod, w_in, b_in, q_gain, k_gain, w_out, b_out))
    return final_state[None]
```

```python
import functools

import jax
import jax.numpy as jnp
from jax import lax
from jax.experimental import pallas as pl
from jax.experimental.pallas import tpu as pltpu
from jax.sharding import PartitionSpec as P

ROPE_SPLIT = (16, 56, 56)
THETA = 256.0
EPS = 1e-6
LOG2E = 1.4426950408889634
HEAD = 128
NDEV = 8
AXES = ('cp', 'sp')


def rope_rows(positions):
    freq_rows = []
    lane = 0
    for width in ROPE_SPLIT:
        freq = THETA ** (-jnp.arange(0, width, 2).astype(jnp.float32) / width)
        freq_rows.append(jnp.pad(jnp.repeat(freq, 2), (lane, HEAD - lane - width)))
        lane += width
    pos = positions.astype(jnp.float32)
    angles = pos[:, 0:1] * freq_rows[0] + pos[:, 1:2] * freq_rows[1] + pos[:, 2:3] * freq_rows[2]
    sign = jnp.where(jnp.arange(HEAD) % 2 == 0, -1.0, 1.0).astype(jnp.float32)
    return jnp.cos(angles), jnp.sin(angles) * sign


def mod_body(idx_ref, c_ref, w_ref, o_ref):
    part = jnp.dot(c_ref[...], w_ref[0], preferred_element_type=jnp.float32)

    @pl.when(pl.program_id(1) == 0)
    def _():
        o_ref[0] = part

    @pl.when(pl.program_id(1) != 0)
    def _():
        o_ref[0] += part


def mod_columns(c_vec, w_mod, my_idx):
    layers, depth, width = w_mod.shape
    cols = width // NDEV
    steps = 4
    rows = depth // steps
    c_pad = jnp.broadcast_to(c_vec, (16, depth))
    out = pl.pallas_call(
        mod_body,
        out_shape=jax.ShapeDtypeStruct((layers, 16, cols), jnp.float32),
        grid_spec=pltpu.PrefetchScalarGridSpec(
            num_scalar_prefetch=1,
            grid=(layers, steps),
            in_specs=[
                pl.BlockSpec((16, rows), lambda l, s, i: (0, s)),
                pl.BlockSpec((1, rows, cols), lambda l, s, i: (l, s, i[0])),
            ],
            out_specs=pl.BlockSpec((1, 16, cols), lambda l, s, i: (l, 0, 0)),
        ),
        cost_estimate=pl.CostEstimate(flops=2 * 16 * layers * depth * cols, bytes_accessed=2 * layers * depth * cols, transcendentals=0),
        name='mod_cols',
    )(my_idx, c_pad, w_mod)
    return out[:, 0]


QW = 512
MW = 1024
QH = QW // HEAD


def device_of(index, sp_size):
    return {'part': lax.axis_index('part'), 'cp': index // sp_size, 'sp': index % sp_size}


def front_body(x_ref, shift_ref, scale_ref, b_ref, bo_ref, g_ref, cos_ref, sin_ref, w_in_ref, w_out_ref,
               recv_ref, y_hbm, h_ref, y_ref, win_ref, wout_ref, send_ref, act_ref,
               in_sem, out_sem, y_sem, send_sem, recv_sem, keep_sem, *, layer, sp_size):
    tokens, dim = x_ref.shape
    q_steps = dim // QW
    mlp_dim = w_out_ref.shape[1] - dim
    m_steps = mlp_dim // MW
    me = lax.axis_index('cp') * sp_size + lax.axis_index('sp')
    halves = NDEV // QH

    def in_copy(col, slot, idx):
        return pltpu.make_async_copy(w_in_ref.at[layer, :, pl.ds(pl.multiple_of(col, QW), QW)], win_ref.at[slot, idx], in_sem.at[slot, idx])

    def out_copy(step, slot):
        return pltpu.make_async_copy(w_out_ref.at[layer, pl.ds(pl.multiple_of(dim + step * MW, MW), MW), :], wout_ref.at[slot], out_sem.at[slot])

    def q_cols(step):
        return [w * dim + step * QW for w in range(3)]

    def m_cols(step):
        return [3 * dim + step * MW + i * QW for i in range(MW // QW)]

    def keep(part):
        return pltpu.make_async_copy(send_ref.at[part * NDEV + me], recv_ref.at[part, me], keep_sem.at[part])

    def send(step):
        part = step // halves
        for dd in range(QH):
            dest = (step % halves) * QH + dd

            @pl.when(dest != me)
            def _():
                pltpu.make_async_remote_copy(
                    src_ref=send_ref.at[part * NDEV + dest], dst_ref=recv_ref.at[part, me],
                    send_sem=send_sem, recv_sem=recv_sem,
                    device_id=device_of(dest, sp_size), device_id_type=pl.DeviceIdType.MESH).start()

            @pl.when(dest == me)
            def _():
                keep(part).start()

    for w, col in enumerate(q_cols(0)):
        in_copy(col, 0, w).start()
    barrier = pltpu.get_barrier_semaphore()
    for k in range(1, NDEV):
        pl.semaphore_signal(barrier, inc=1, device_id=device_of((me + k) % NDEV, sp_size), device_id_type=pl.DeviceIdType.MESH)

    rows = 16
    scale_p = 1.0 + scale_ref[...]
    shift = shift_ref[...]
    bias_out = jnp.broadcast_to(bo_ref[...], (rows, dim))

    def norm_rows(r, carry):
        at = pl.ds(pl.multiple_of(r * rows, rows), rows)
        v = x_ref[at, :].astype(jnp.float32)
        v = v - jnp.mean(v, axis=-1, keepdims=True)
        var = jnp.mean(v * v, axis=-1, keepdims=True)
        h_ref[at, :] = (v * lax.rsqrt(var + EPS) * scale_p + shift).astype(jnp.bfloat16)
        y_ref[at, :] = bias_out
        return carry

    lax.fori_loop(0, tokens // rows, norm_rows, 0)

    even = lax.broadcasted_iota(jnp.int32, (1, HEAD), 1) % 2 == 0

    def project(slot, idx, col):
        acc = jnp.dot(h_ref[...], win_ref[slot, idx], preferred_element_type=jnp.float32)
        return (acc + b_ref[:, pl.ds(pl.multiple_of(col, QW), QW)]).astype(jnp.bfloat16)

    def q_step(t, carry):
        slot = t % 2
        for w, col in enumerate(q_cols(t)):
            in_copy(col, slot, w).wait()

        @pl.when(t + 1 < q_steps)
        def _():
            for w, col in enumerate(q_cols(t + 1)):
                in_copy(col, 1 - slot, w).start()

        @pl.when(t + 1 == q_steps)
        def _():
            for i, col in enumerate(m_cols(0)):
                in_copy(col, 1 - slot, i).start()
            out_copy(0, 1 - slot).start()

        @pl.when(t == 1)
        def _():
            pl.semaphore_wait(barrier, NDEV - 1)

        @pl.when(t > 0)
        def _():
            send(t - 1)

        for w, col in enumerate(q_cols(t)):
            u = project(slot, w, col)
            for n in range(QH):
                piece = u[:, n * HEAD:(n + 1) * HEAD]
                if w < 2:
                    v = piece.astype(jnp.float32)
                    v = v * lax.rsqrt(jnp.mean(v * v, axis=-1, keepdims=True) + EPS) * g_ref[w:w + 1, :]
                    swapped = jnp.where(even, pltpu.roll(v, HEAD - 1, 1), pltpu.roll(v, 1, 1))
                    piece = (v * cos_ref[...] + swapped * sin_ref[...]).astype(jnp.bfloat16)
                send_ref[t * QH + n, w] = piece
        return carry

    lax.fori_loop(0, q_steps, q_step, 0)

    def m_step(b, carry):
        slot = (q_steps + b) % 2
        for i, col in enumerate(m_cols(b)):
            in_copy(col, slot, i).wait()
        out_copy(b, slot).wait()

        @pl.when(b + 1 < m_steps)
        def _():
            for i, col in enumerate(m_cols(b + 1)):
                in_copy(col, 1 - slot, i).start()
            out_copy(b + 1, 1 - slot).start()

        @pl.when(b == 0)
        def _():
            send(q_steps - 1)

        for i, col in enumerate(m_cols(b)):
            v = project(slot, i, col).astype(jnp.float32)
            inner = v * (0.7978845608028654 + (0.7978845608028654 * 0.044715) * (v * v))
            half = 0.5 * v
            act_ref[i] = (half + half * jnp.tanh(inner)).astype(jnp.bfloat16)
        for i in range(MW // QW):
            y_ref[...] += jnp.dot(act_ref[i], wout_ref[slot, i * QW:(i + 1) * QW, :], preferred_element_type=jnp.float32)
        return carry

    lax.fori_loop(0, m_steps, m_step, 0)
    y_copy = pltpu.make_async_copy(y_ref, y_hbm, y_sem)
    y_copy.start()
    parts = q_steps // halves
    moved = send_ref.at[pl.ds(0, parts * (NDEV - 1))]
    pltpu.make_async_copy(moved, moved, send_sem).wait()
    pltpu.make_async_copy(moved, moved, recv_sem).wait()
    for part in range(parts):
        keep(part).wait()
    y_copy.wait()


def front(state, shift_row, scale_row, b_in_row, b_out_row, gains, cos_t, sin_t, w_in, w_out, layer, sp_size):
    tokens, dim = state.shape
    mlp_dim = w_out.shape[1] - dim
    vmem = pl.BlockSpec(memory_space=pltpu.VMEM)
    hbm = pl.BlockSpec(memory_space=pl.ANY)
    parts = dim // (NDEV * HEAD)
    flops = 2 * tokens * dim * (3 * dim + 2 * mlp_dim)
    return pl.pallas_call(
        functools.partial(front_body, layer=layer, sp_size=sp_size),
        out_shape=(jax.ShapeDtypeStruct((parts, NDEV, 3, tokens, HEAD), jnp.bfloat16),
                   jax.ShapeDtypeStruct((tokens, dim), jnp.float32)),
        in_specs=[vmem] * 8 + [hbm, hbm],
        out_specs=(hbm, hbm),
        scratch_shapes=[
            pltpu.VMEM((tokens, dim), jnp.bfloat16),
            pltpu.VMEM((tokens, dim), jnp.float32),
            pltpu.VMEM((2, 3, dim, QW), jnp.bfloat16),
            pltpu.VMEM((2, MW, dim), jnp.bfloat16),
            pltpu.VMEM((parts * NDEV, 3, tokens, HEAD), jnp.bfloat16),
            pltpu.VMEM((MW // QW, tokens, QW), jnp.bfloat16),
            pltpu.SemaphoreType.DMA((2, 3)),
            pltpu.SemaphoreType.DMA((2,)),
            pltpu.SemaphoreType.DMA,
            pltpu.SemaphoreType.DMA,
            pltpu.SemaphoreType.DMA,
            pltpu.SemaphoreType.DMA((parts,)),
        ],
        compiler_params=pltpu.CompilerParams(collective_id=layer, has_side_effects=True, vmem_limit_bytes=62 * 1024 * 1024),
        cost_estimate=pl.CostEstimate(flops=flops, bytes_accessed=2 * dim * (3 * dim + 2 * mlp_dim), transcendentals=tokens * mlp_dim),
        name=f'front{layer}',
    )(state, shift_row, scale_row, b_in_row, b_out_row, gains, cos_t, sin_t, w_in, w_out)


def attn_body(x_ref, mask_ref, o_ref, vt_ref, *, q_chunks, k_chunks):
    chunks = x_ref.shape[0]
    tokens = x_ref.shape[2]
    step = pl.program_id(0)
    factor = (HEAD ** -0.5) * LOG2E

    @pl.when(step == 0)
    def _():
        for c in range(chunks):
            vt_ref[:, c * tokens:(c + 1) * tokens] = x_ref[c, 2].T

    q_rows = q_chunks * tokens
    q_t = x_ref[pl.ds(step * q_chunks, q_chunks), 0].reshape(q_rows, HEAD).T
    k_rows = k_chunks * tokens
    m = jnp.full((1, q_rows), -1e30, jnp.float32)
    l = jnp.zeros((1, q_rows), jnp.float32)
    acc = jnp.zeros((HEAD, q_rows), jnp.float32)
    for c in range(chunks // k_chunks):
        keys = x_ref[c * k_chunks:(c + 1) * k_chunks, 1].reshape(k_rows, HEAD)
        s = jnp.dot(keys, q_t, preferred_element_type=jnp.float32)
        if (c + 1) * k_chunks == chunks:
            s = jnp.where(mask_ref[...] > 0, s, -1e30)
        new_m = jnp.maximum(m, jnp.max(s, axis=0, keepdims=True))
        alpha = jnp.exp2((m - new_m) * factor)
        p = jnp.exp2((s - new_m) * factor)
        l = l * alpha + jnp.sum(p, axis=0, keepdims=True)
        pv = jnp.dot(vt_ref[:, c * k_rows:(c + 1) * k_rows], p.astype(jnp.bfloat16), preferred_element_type=jnp.float32)
        acc = acc * alpha + pv
        m = new_m
    out = (acc / l).T.astype(jnp.bfloat16)
    o_ref[...] = out.reshape(q_chunks, tokens, HEAD)


def attend(recv, key_ok, part):
    _, chunks, _, tokens, _ = recv.shape
    q_chunks = 2
    k_chunks = 2
    steps = chunks // q_chunks
    seq = chunks * tokens
    return pl.pallas_call(
        functools.partial(attn_body, q_chunks=q_chunks, k_chunks=k_chunks),
        out_shape=jax.ShapeDtypeStruct((chunks, tokens, HEAD), jnp.bfloat16),
        grid=(steps,),
        in_specs=[
            pl.BlockSpec((None,) + recv.shape[1:], lambda s: (part, 0, 0, 0, 0)),
            pl.BlockSpec((k_chunks * tokens, 1), lambda s: (0, 0)),
        ],
        out_specs=pl.BlockSpec((q_chunks, tokens, HEAD), lambda s: (s, 0, 0)),
        scratch_shapes=[pltpu.VMEM((HEAD, seq), jnp.bfloat16)],
        cost_estimate=pl.CostEstimate(flops=8 * seq * seq * HEAD, bytes_accessed=8 * seq * HEAD, transcendentals=seq * seq),
        name=f'attend{part}',
    )(recv, key_ok)


def out_body(a0_ref, a1_ref, a2_ref, w_ref, y_ref, g_ref, x_ref, o_ref, a_ref):
    @pl.when(pl.program_id(0) == 0)
    def _():
        for j, part_ref in enumerate((a0_ref, a1_ref, a2_ref)):
            for d in range(NDEV):
                col = (j * NDEV + d) * HEAD
                a_ref[:, col:col + HEAD] = part_ref[d]

    y = jnp.dot(a_ref[...], w_ref[0], preferred_element_type=jnp.float32) + y_ref[...]
    o_ref[...] = (x_ref[...].astype(jnp.float32) + g_ref[...] * y).astype(jnp.bfloat16)


def output_step(attn, w_out, y_mlp, gate_row, state, layer):
    tokens, dim = state.shape
    width = 512
    part_spec = pl.BlockSpec((NDEV, tokens, HEAD), lambda n: (0, 0, 0))
    row_spec = pl.BlockSpec((1, width), lambda n: (0, n))
    tok_spec = pl.BlockSpec((tokens, width), lambda n: (0, n))
    return pl.pallas_call(
        out_body,
        out_shape=jax.ShapeDtypeStruct((tokens, dim), jnp.bfloat16),
        grid=(dim // width,),
        in_specs=[part_spec, part_spec, part_spec,
                  pl.BlockSpec((1, dim, width), lambda n: (layer, 0, n)),
                  tok_spec, row_spec, tok_spec],
        out_specs=tok_spec,
        scratch_shapes=[pltpu.VMEM((tokens, dim), jnp.bfloat16)],
        cost_estimate=pl.CostEstimate(flops=2 * tokens * dim * dim, bytes_accessed=2 * dim * dim, transcendentals=0),
        name='out_step',
    )(*attn, w_out, y_mlp, gate_row, state)


def solution(mesh):
    tok_spec = P('part', AXES, None)
    mask_spec = P('part', AXES)
    vec_spec = P('part', None)
    rep = P()

    def local_blocks(hidden, valid_mask, positions, cond_vec, w_mod, b_mod, w_in, b_in, q_gain, k_gain, w_out, b_out):
        dim = hidden.shape[-1]
        tokens = hidden.shape[1]
        layers = w_in.shape[0]
        my_idx = (lax.axis_index('cp') * mesh.shape['sp'] + lax.axis_index('sp')).astype(jnp.int32).reshape(1)
        cos_t, sin_t = rope_rows(positions[0])
        c_vec = jax.nn.silu(cond_vec).astype(jnp.bfloat16)
        mod_loc = mod_columns(c_vec, w_mod, my_idx)
        packed = jnp.concatenate([mod_loc.reshape(1, -1), valid_mask.astype(jnp.float32)], axis=1)
        gathered = lax.all_gather(packed, AXES, tiled=True)
        mods = gathered[:, :-tokens].reshape(NDEV, layers, -1)
        mods = jnp.swapaxes(mods, 0, 1).reshape(layers, 1, 3 * dim) + b_mod.astype(jnp.float32)[:, None]
        key_ok = gathered[NDEV - 2:, -tokens:].reshape(2 * tokens, 1)
        b_in_f = b_in.astype(jnp.float32)
        b_out_f = b_out.astype(jnp.float32)
        state = hidden[0]
        for layer in range(layers):
            shift_row = mods[layer, :, :dim]
            scale_row = mods[layer, :, dim:2 * dim]
            gate_row = mods[layer, :, 2 * dim:]
            gains = jnp.stack([q_gain[layer], k_gain[layer]]).astype(jnp.float32)
            recv, y_mlp = front(state, shift_row, scale_row, b_in_f[layer:layer + 1], b_out_f[layer:layer + 1], gains, cos_t, sin_t, w_in, w_out, layer, mesh.shape['sp'])
            outs = [attend(recv, key_ok, j) for j in range(recv.shape[0])]
            back = [lax.all_to_all(o, AXES, 0, 0, tiled=True) for o in outs]
            state = output_step(back, w_out, y_mlp, gate_row, state, layer)
        return state[None]

    in_specs = (tok_spec, mask_spec, tok_spec, vec_spec, rep, rep, rep, rep, rep, rep, rep, rep)
    return jax.shard_map(local_blocks, mesh=mesh, in_specs=in_specs, out_specs=tok_spec, check_vma=False)
```

```python
import functools

import jax
import jax.numpy as jnp
from jax import lax
from jax.experimental import pallas as pl
from jax.experimental.pallas import tpu as pltpu
from jax.sharding import PartitionSpec as P

ROPE_SPLIT = (16, 56, 56)
THETA = 256.0
EPS = 1e-6
LOG2E = 1.4426950408889634
HEAD = 128
NDEV = 8
AXES = ('cp', 'sp')


def rope_rows(positions):
    freq_rows = []
    lane = 0
    for width in ROPE_SPLIT:
        freq = THETA ** (-jnp.arange(0, width, 2).astype(jnp.float32) / width)
        freq_rows.append(jnp.pad(jnp.repeat(freq, 2), (lane, HEAD - lane - width)))
        lane += width
    pos = positions.astype(jnp.float32)
    angles = pos[:, 0:1] * freq_rows[0] + pos[:, 1:2] * freq_rows[1] + pos[:, 2:3] * freq_rows[2]
    sign = jnp.where(jnp.arange(HEAD) % 2 == 0, -1.0, 1.0).astype(jnp.float32)
    return jnp.cos(angles), jnp.sin(angles) * sign


def mod_body(idx_ref, c_ref, w_ref, o_ref):
    part = jnp.dot(c_ref[...], w_ref[0], preferred_element_type=jnp.float32)

    @pl.when(pl.program_id(1) == 0)
    def _():
        o_ref[0] = part

    @pl.when(pl.program_id(1) != 0)
    def _():
        o_ref[0] += part


def mod_columns(c_vec, w_mod, my_idx):
    layers, depth, width = w_mod.shape
    cols = width // NDEV
    steps = 4
    rows = depth // steps
    c_pad = jnp.broadcast_to(c_vec, (16, depth))
    out = pl.pallas_call(
        mod_body,
        out_shape=jax.ShapeDtypeStruct((layers, 16, cols), jnp.float32),
        grid_spec=pltpu.PrefetchScalarGridSpec(
            num_scalar_prefetch=1,
            grid=(layers, steps),
            in_specs=[
                pl.BlockSpec((16, rows), lambda l, s, i: (0, s)),
                pl.BlockSpec((1, rows, cols), lambda l, s, i: (l, s, i[0])),
            ],
            out_specs=pl.BlockSpec((1, 16, cols), lambda l, s, i: (l, 0, 0)),
        ),
        cost_estimate=pl.CostEstimate(flops=2 * 16 * layers * depth * cols, bytes_accessed=2 * layers * depth * cols, transcendentals=0),
        name='mod_cols',
    )(my_idx, c_pad, w_mod)
    return out[:, 0]


QW = 512
MW = 1024
QH = QW // HEAD


def device_of(index, sp_size):
    return {'part': lax.axis_index('part'), 'cp': index // sp_size, 'sp': index % sp_size}


def front_body(x_ref, shift_ref, scale_ref, b_ref, bo_ref, g_ref, cos_ref, sin_ref, w_in_ref, w_out_ref,
               recv_ref, y_hbm, h_ref, y_ref, win_ref, wout_ref, send_ref, act_ref,
               in_sem, out_sem, y_sem, send_sem, recv_sem, keep_sem, *, layer, sp_size):
    tokens, dim = x_ref.shape
    q_steps = dim // QW
    mlp_dim = w_out_ref.shape[1] - dim
    m_steps = mlp_dim // MW
    me = lax.axis_index('cp') * sp_size + lax.axis_index('sp')
    halves = NDEV // QH

    def in_copy(col, slot, idx):
        return pltpu.make_async_copy(w_in_ref.at[layer, :, pl.ds(pl.multiple_of(col, QW), QW)], win_ref.at[slot, idx], in_sem.at[slot, idx])

    def out_copy(step, slot):
        return pltpu.make_async_copy(w_out_ref.at[layer, pl.ds(pl.multiple_of(dim + step * MW, MW), MW), :], wout_ref.at[slot], out_sem.at[slot])

    def q_cols(step):
        return [w * dim + step * QW for w in range(3)]

    def m_cols(step):
        return [3 * dim + step * MW + i * QW for i in range(MW // QW)]

    def landing(part):
        return recv_ref.at[part, :, pl.ds(pl.multiple_of(me * tokens, tokens), tokens), :]

    def keep(part):
        return pltpu.make_async_copy(send_ref.at[part * NDEV + me], landing(part), keep_sem.at[part])

    def send(step):
        part = step // halves
        for dd in range(QH):
            dest = (step % halves) * QH + dd

            @pl.when(dest != me)
            def _():
                pltpu.make_async_remote_copy(
                    src_ref=send_ref.at[part * NDEV + dest], dst_ref=landing(part),
                    send_sem=send_sem, recv_sem=recv_sem,
                    device_id=device_of(dest, sp_size), device_id_type=pl.DeviceIdType.MESH).start()

            @pl.when(dest == me)
            def _():
                keep(part).start()

    for w, col in enumerate(q_cols(0)):
        in_copy(col, 0, w).start()
    barrier = pltpu.get_barrier_semaphore()
    for k in range(1, NDEV):
        pl.semaphore_signal(barrier, inc=1, device_id=device_of((me + k) % NDEV, sp_size), device_id_type=pl.DeviceIdType.MESH)

    rows = 16
    scale_p = 1.0 + scale_ref[...]
    shift = shift_ref[...]
    bias_out = jnp.broadcast_to(bo_ref[...], (rows, dim))

    def norm_rows(r, carry):
        at = pl.ds(pl.multiple_of(r * rows, rows), rows)
        v = x_ref[at, :].astype(jnp.float32)
        v = v - jnp.mean(v, axis=-1, keepdims=True)
        var = jnp.mean(v * v, axis=-1, keepdims=True)
        h_ref[at, :] = (v * lax.rsqrt(var + EPS) * scale_p + shift).astype(jnp.bfloat16)
        y_ref[at, :] = bias_out
        return carry

    lax.fori_loop(0, tokens // rows, norm_rows, 0)

    even = lax.broadcasted_iota(jnp.int32, (1, HEAD), 1) % 2 == 0

    def project(slot, idx, col):
        acc = jnp.dot(h_ref[...], win_ref[slot, idx], preferred_element_type=jnp.float32)
        return (acc + b_ref[:, pl.ds(pl.multiple_of(col, QW), QW)]).astype(jnp.bfloat16)

    def q_step(t, carry):
        slot = t % 2
        for w, col in enumerate(q_cols(t)):
            in_copy(col, slot, w).wait()

        @pl.when(t + 1 < q_steps)
        def _():
            for w, col in enumerate(q_cols(t + 1)):
                in_copy(col, 1 - slot, w).start()

        @pl.when(t + 1 == q_steps)
        def _():
            for i, col in enumerate(m_cols(0)):
                in_copy(col, 1 - slot, i).start()
            out_copy(0, 1 - slot).start()

        @pl.when(t == 1)
        def _():
            pl.semaphore_wait(barrier, NDEV - 1)

        @pl.when(t > 0)
        def _():
            send(t - 1)

        for w, col in enumerate(q_cols(t)):
            u = project(slot, w, col)
            for n in range(QH):
                piece = u[:, n * HEAD:(n + 1) * HEAD]
                if w < 2:
                    v = piece.astype(jnp.float32)
                    v = v * lax.rsqrt(jnp.mean(v * v, axis=-1, keepdims=True) + EPS) * g_ref[w:w + 1, :]
                    swapped = jnp.where(even, pltpu.roll(v, HEAD - 1, 1), pltpu.roll(v, 1, 1))
                    piece = (v * cos_ref[...] + swapped * sin_ref[...]).astype(jnp.bfloat16)
                send_ref[t * QH + n, w] = piece
        return carry

    lax.fori_loop(0, q_steps, q_step, 0)

    def m_step(b, carry):
        slot = (q_steps + b) % 2
        for i, col in enumerate(m_cols(b)):
            in_copy(col, slot, i).wait()
        out_copy(b, slot).wait()

        @pl.when(b + 1 < m_steps)
        def _():
            for i, col in enumerate(m_cols(b + 1)):
                in_copy(col, 1 - slot, i).start()
            out_copy(b + 1, 1 - slot).start()

        @pl.when(b == 0)
        def _():
            send(q_steps - 1)

        for i, col in enumerate(m_cols(b)):
            v = project(slot, i, col).astype(jnp.float32)
            inner = v * (0.7978845608028654 + (0.7978845608028654 * 0.044715) * (v * v))
            half = 0.5 * v
            act_ref[i] = (half + half * jnp.tanh(inner)).astype(jnp.bfloat16)
        for i in range(MW // QW):
            y_ref[...] += jnp.dot(act_ref[i], wout_ref[slot, i * QW:(i + 1) * QW, :], preferred_element_type=jnp.float32)
        return carry

    lax.fori_loop(0, m_steps, m_step, 0)
    y_copy = pltpu.make_async_copy(y_ref, y_hbm, y_sem)
    y_copy.start()
    parts = q_steps // halves
    moved = send_ref.at[pl.ds(0, parts * (NDEV - 1))]
    pltpu.make_async_copy(moved, moved, send_sem).wait()
    pltpu.make_async_copy(moved, moved, recv_sem).wait()
    for part in range(parts):
        keep(part).wait()
    y_copy.wait()


def front(state, shift_row, scale_row, b_in_row, b_out_row, gains, cos_t, sin_t, w_in, w_out, layer, sp_size):
    tokens, dim = state.shape
    mlp_dim = w_out.shape[1] - dim
    vmem = pl.BlockSpec(memory_space=pltpu.VMEM)
    hbm = pl.BlockSpec(memory_space=pl.ANY)
    parts = dim // (NDEV * HEAD)
    flops = 2 * tokens * dim * (3 * dim + 2 * mlp_dim)
    return pl.pallas_call(
        functools.partial(front_body, layer=layer, sp_size=sp_size),
        out_shape=(jax.ShapeDtypeStruct((parts, 3, NDEV * tokens, HEAD), jnp.bfloat16),
                   jax.ShapeDtypeStruct((tokens, dim), jnp.float32)),
        in_specs=[vmem] * 8 + [hbm, hbm],
        out_specs=(hbm, hbm),
        scratch_shapes=[
            pltpu.VMEM((tokens, dim), jnp.bfloat16),
            pltpu.VMEM((tokens, dim), jnp.float32),
            pltpu.VMEM((2, 3, dim, QW), jnp.bfloat16),
            pltpu.VMEM((2, MW, dim), jnp.bfloat16),
            pltpu.VMEM((parts * NDEV, 3, tokens, HEAD), jnp.bfloat16),
            pltpu.VMEM((MW // QW, tokens, QW), jnp.bfloat16),
            pltpu.SemaphoreType.DMA((2, 3)),
            pltpu.SemaphoreType.DMA((2,)),
            pltpu.SemaphoreType.DMA,
            pltpu.SemaphoreType.DMA,
            pltpu.SemaphoreType.DMA,
            pltpu.SemaphoreType.DMA((parts,)),
        ],
        compiler_params=pltpu.CompilerParams(collective_id=layer, has_side_effects=True, vmem_limit_bytes=62 * 1024 * 1024),
        cost_estimate=pl.CostEstimate(flops=flops, bytes_accessed=2 * dim * (3 * dim + 2 * mlp_dim), transcendentals=tokens * mlp_dim),
        name=f'front{layer}',
    )(state, shift_row, scale_row, b_in_row, b_out_row, gains, cos_t, sin_t, w_in, w_out)


KC = 512


def back_body(recv_ref, mask_ref, gate_ref, x_hbm, y_hbm, w_hbm, o_ref,
              kv_ref, vt_ref, qt_ref, s_ref, p_ref, send_ref, a_ref, x_ref, y_ref, w_ref,
              kv_sem, load_sem, send_sem, recv_sem, keep_sem, *, layer, sp_size):
    tokens, dim = o_ref.shape
    parts, _, seq, _ = recv_ref.shape
    me = lax.axis_index('cp') * sp_size + lax.axis_index('sp')
    chips = NDEV // 2
    q_rows = seq // chips
    steps = parts * chips
    factor = (HEAD ** -0.5) * LOG2E

    def kv_copy(part, slot):
        return pltpu.make_async_copy(recv_ref.at[part], kv_ref.at[slot], kv_sem.at[slot])

    loads = [
        pltpu.make_async_copy(w_hbm.at[layer, pl.ds(0, dim), :], w_ref, load_sem.at[0]),
        pltpu.make_async_copy(y_hbm, y_ref, load_sem.at[1]),
        pltpu.make_async_copy(x_hbm, x_ref, load_sem.at[2]),
    ]
    kv_copy(0, 0).start()
    barrier = pltpu.get_barrier_semaphore()
    for k in range(1, NDEV):
        pl.semaphore_signal(barrier, inc=1, device_id=device_of((me + k) % NDEV, sp_size), device_id_type=pl.DeviceIdType.MESH)

    def chip_at(t):
        return (me // 2 + 1 + t % chips) % chips

    def landing(part):
        return a_ref.at[:, pl.ds(pl.multiple_of((part * NDEV + me) * HEAD, HEAD), HEAD)]

    def keep(part):
        return pltpu.make_async_copy(send_ref.at[part * NDEV + me], landing(part), keep_sem.at[part])

    def send(t):
        part = t // chips
        for core in range(2):
            dest = chip_at(t) * 2 + core

            @pl.when(dest != me)
            def _():
                pltpu.make_async_remote_copy(
                    src_ref=send_ref.at[part * NDEV + dest], dst_ref=landing(part),
                    send_sem=send_sem, recv_sem=recv_sem.at[part],
                    device_id=device_of(dest, sp_size), device_id_type=pl.DeviceIdType.MESH).start()

            @pl.when(dest == me)
            def _():
                keep(part).start()

    def attend(t, carry):
        part = t // chips
        slot = part % 2
        chip = chip_at(t)

        @pl.when(t % chips == 0)
        def _():
            kv_copy(part, slot).wait()

            @pl.when(part + 1 < parts)
            def _():
                kv_copy(part + 1, 1 - slot).start()

            for c in range(seq // KC):
                vt_ref[:, c * KC:(c + 1) * KC] = kv_ref[slot, 2, c * KC:(c + 1) * KC, :].T

        @pl.when(t == 1)
        def _():
            pl.semaphore_wait(barrier, NDEV - 1)

        @pl.when(t > 0)
        def _():
            send(t - 1)

        qt_ref[...] = kv_ref[slot, 0, pl.ds(pl.multiple_of(chip * q_rows, q_rows), q_rows), :].T

        blocks = seq // KC
        maxes = [jnp.full((1, q_rows), -1e30, jnp.float32)]

        def scores(c):
            s = jnp.dot(kv_ref[slot, 1, c * KC:(c + 1) * KC, :], qt_ref[...], preferred_element_type=jnp.float32)
            if c + 1 == blocks:
                s = jnp.where(jnp.concatenate([mask_ref[...]] * (q_rows // HEAD), axis=1) > 0, s, -1e30)
            s_ref[c % 2] = s
            maxes.append(jnp.maximum(maxes[-1], jnp.max(s, axis=0, keepdims=True)))

        total = jnp.zeros((1, q_rows), jnp.float32)
        acc = None
        scores(0)
        for c in range(blocks):
            if c + 1 < blocks:
                scores(c + 1)
            p = jnp.exp2((s_ref[c % 2] - maxes[c + 1]) * factor)
            alpha = jnp.exp2((maxes[c] - maxes[c + 1]) * factor)
            total = total * alpha + jnp.sum(p, axis=0, keepdims=True)
            p_ref[c % 2] = p.astype(jnp.bfloat16)
            pv = jnp.dot(vt_ref[:, c * KC:(c + 1) * KC], p_ref[c % 2], preferred_element_type=jnp.float32)
            acc = pv if acc is None else acc * alpha + pv
        out = (acc * (1.0 / total)).astype(jnp.bfloat16).T
        for core in range(2):
            send_ref[part * NDEV + chip * 2 + core] = out[core * tokens:(core + 1) * tokens]
        return carry

    for load in loads:
        load.start()
    lax.fori_loop(0, steps, attend, 0)
    send(steps - 1)

    def arrived(part):
        moved = send_ref.at[pl.ds(0, NDEV - 1)]
        pltpu.make_async_copy(moved, moved, recv_sem.at[part]).wait()
        keep(part).wait()

    for load in loads:
        load.wait()
    for part in range(parts - 1):
        arrived(part)
    split = (parts - 1) * NDEV * HEAD
    for n in range(0, dim, QW):
        y_ref[:, n:n + QW] += jnp.dot(a_ref[:, :split], w_ref[:split, n:n + QW], preferred_element_type=jnp.float32)
    arrived(parts - 1)
    for n in range(0, dim, QW):
        y = y_ref[:, n:n + QW] + jnp.dot(a_ref[:, split:], w_ref[split:, n:n + QW], preferred_element_type=jnp.float32)
        o_ref[:, n:n + QW] = (x_ref[:, n:n + QW].astype(jnp.float32) + gate_ref[:, n:n + QW] * y).astype(jnp.bfloat16)
    moved = send_ref.at[pl.ds(0, parts * (NDEV - 1))]
    pltpu.make_async_copy(moved, moved, send_sem).wait()


def back(recv, key_ok, gate_row, state, y_mlp, w_out, layer, sp_size):
    tokens, dim = state.shape
    parts, _, seq, _ = recv.shape
    q_rows = seq // (NDEV // 2)
    vmem = pl.BlockSpec(memory_space=pltpu.VMEM)
    hbm = pl.BlockSpec(memory_space=pl.ANY)
    return pl.pallas_call(
        functools.partial(back_body, layer=layer, sp_size=sp_size),
        out_shape=jax.ShapeDtypeStruct((tokens, dim), jnp.bfloat16),
        in_specs=[hbm, vmem, vmem, hbm, hbm, hbm],
        out_specs=vmem,
        scratch_shapes=[
            pltpu.VMEM((2, 3, seq, HEAD), jnp.bfloat16),
            pltpu.VMEM((HEAD, seq), jnp.bfloat16),
            pltpu.VMEM((HEAD, q_rows), jnp.bfloat16),
            pltpu.VMEM((2, KC, q_rows), jnp.float32),
            pltpu.VMEM((2, KC, q_rows), jnp.bfloat16),
            pltpu.VMEM((parts * NDEV, tokens, HEAD), jnp.bfloat16),
            pltpu.VMEM((tokens, dim), jnp.bfloat16),
            pltpu.VMEM((tokens, dim), jnp.bfloat16),
            pltpu.VMEM((tokens, dim), jnp.float32),
            pltpu.VMEM((dim, dim), jnp.bfloat16),
            pltpu.SemaphoreType.DMA((2,)),
            pltpu.SemaphoreType.DMA((3,)),
            pltpu.SemaphoreType.DMA,
            pltpu.SemaphoreType.DMA((parts,)),
            pltpu.SemaphoreType.DMA((parts,)),
        ],
        compiler_params=pltpu.CompilerParams(collective_id=8 + layer, has_side_effects=True, vmem_limit_bytes=62 * 1024 * 1024),
        cost_estimate=pl.CostEstimate(flops=4 * parts * seq * seq * HEAD + 2 * tokens * dim * dim, bytes_accessed=2 * dim * dim, transcendentals=parts * seq * seq),
        name=f'back{layer}',
    )(recv, key_ok, gate_row, state, y_mlp, w_out)


def solution(mesh):
    tok_spec = P('part', AXES, None)
    mask_spec = P('part', AXES)
    vec_spec = P('part', None)
    rep = P()

    def local_blocks(hidden, valid_mask, positions, cond_vec, w_mod, b_mod, w_in, b_in, q_gain, k_gain, w_out, b_out):
        dim = hidden.shape[-1]
        tokens = hidden.shape[1]
        layers = w_in.shape[0]
        my_idx = (lax.axis_index('cp') * mesh.shape['sp'] + lax.axis_index('sp')).astype(jnp.int32).reshape(1)
        cos_t, sin_t = rope_rows(positions[0])
        c_vec = jax.nn.silu(cond_vec).astype(jnp.bfloat16)
        mod_loc = mod_columns(c_vec, w_mod, my_idx)
        packed = jnp.concatenate([mod_loc.reshape(1, -1), valid_mask.astype(jnp.float32)], axis=1)
        gathered = lax.all_gather(packed, AXES, tiled=True)
        mods = gathered[:, :-tokens].reshape(NDEV, layers, -1)
        mods = jnp.swapaxes(mods, 0, 1).reshape(layers, 1, 3 * dim) + b_mod.astype(jnp.float32)[:, None]
        key_ok = jnp.broadcast_to(gathered[:, -tokens:].reshape(NDEV * tokens, 1)[-KC:], (KC, HEAD))
        b_in_f = b_in.astype(jnp.float32)
        b_out_f = b_out.astype(jnp.float32)
        state = hidden[0]
        for layer in range(layers):
            shift_row = mods[layer, :, :dim]
            scale_row = mods[layer, :, dim:2 * dim]
            gate_row = mods[layer, :, 2 * dim:]
            gains = jnp.stack([q_gain[layer], k_gain[layer]]).astype(jnp.float32)
            recv, y_mlp = front(state, shift_row, scale_row, b_in_f[layer:layer + 1], b_out_f[layer:layer + 1], gains, cos_t, sin_t, w_in, w_out, layer, mesh.shape['sp'])
            state = back(recv, key_ok, gate_row, state, y_mlp, w_out, layer, mesh.shape['sp'])
        return state[None]

    in_specs = (tok_spec, mask_spec, tok_spec, vec_spec, rep, rep, rep, rep, rep, rep, rep, rep)
    return jax.shard_map(local_blocks, mesh=mesh, in_specs=in_specs, out_specs=tok_spec, check_vma=False)
```

```python
import functools

import jax
import jax.numpy as jnp
from jax import lax
from jax.experimental import pallas as pl
from jax.experimental.pallas import tpu as pltpu
from jax.sharding import PartitionSpec as P

ROPE_SPLIT = (16, 56, 56)
LOG2_THETA = 8.0
EPS = 1e-6
LOG2E = 1.4426950408889634
HEAD = 128
NDEV = 8
AXES = ('cp', 'sp')


def device_of(index, sp_size):
    return {'part': lax.axis_index('part'), 'cp': index // sp_size, 'sp': index % sp_size}


def meet_all(me, sp_size):
    barrier = pltpu.get_barrier_semaphore()
    for k in range(1, NDEV):
        pl.semaphore_signal(barrier, inc=1, device_id=device_of((me + k) % NDEV, sp_size), device_id_type=pl.DeviceIdType.MESH)
    return barrier


MASK_ROW = 2
K_CUT = 3


def mods_body(cond_ref, pos_ref, mask_ref, b_ref, w_hbm, mods_ref, cos_ref, sin_ref, w_ref, stage_ref, w_sem, send_sem, recv_sem, *, sp_size):
    layers, depth, cols = w_ref.shape
    me = lax.axis_index('cp') * sp_size + lax.axis_index('sp')
    mine = pl.ds(pl.multiple_of(me * cols, HEAD), cols)
    cut = depth // K_CUT

    def w_copy(layer, k):
        rows = pl.ds(k * cut, cut)
        return pltpu.make_async_copy(w_hbm.at[layer, rows, mine], w_ref.at[layer, rows, :], w_sem.at[layer, k])

    for layer in range(layers):
        for k in range(K_CUT):
            w_copy(layer, k).start()
    barrier = meet_all(me, sp_size)

    lane = lax.broadcasted_iota(jnp.int32, (1, HEAD), 1)
    angles = None
    start = 0
    for axis_idx, width in enumerate(ROPE_SPLIT):
        pair = ((lane - start) // 2).astype(jnp.float32)
        freq = jnp.exp2(pair * (-2.0 * LOG2_THETA / width))
        freq = jnp.where((lane >= start) & (lane < start + width), freq, 0.0)
        term = pos_ref[:, axis_idx:axis_idx + 1].astype(jnp.float32) * freq
        angles = term if angles is None else angles + term
        start += width
    cos_ref[...] = jnp.cos(angles)
    sine = jnp.sin(angles)
    sin_ref[...] = jnp.where(lane % 2 == 0, -sine, sine)

    cond = cond_ref[...]
    c_vec = jnp.broadcast_to(cond * jax.nn.sigmoid(cond), (16, depth)).astype(jnp.bfloat16)
    stage_ref[...] = jnp.zeros_like(stage_ref)
    stage_ref[MASK_ROW:MASK_ROW + 1, :mask_ref.shape[1]] = mask_ref[...].astype(jnp.float32)
    for layer in range(layers):
        acc = None
        for k in range(K_CUT):
            w_copy(layer, k).wait()
            part = jnp.dot(c_vec[:, k * cut:(k + 1) * cut], w_ref[layer, k * cut:(k + 1) * cut, :], preferred_element_type=jnp.float32)
            acc = part if acc is None else acc + part
        stage_ref[layer:layer + 1, :] = acc[0:1] + b_ref[:, mine].astype(jnp.float32)[layer:layer + 1]
    mods_ref[:, mine] = stage_ref[...]
    pl.semaphore_wait(barrier, NDEV - 1)
    sends = [
        pltpu.make_async_remote_copy(
            src_ref=stage_ref, dst_ref=mods_ref.at[:, mine], send_sem=send_sem.at[k - 1], recv_sem=recv_sem.at[k - 1],
            device_id=device_of((me + k) % NDEV, sp_size), device_id_type=pl.DeviceIdType.MESH)
        for k in range(1, NDEV)
    ]
    for copy in sends:
        copy.start()
    for copy in sends:
        copy.wait()


def modulation(cond_vec, positions, valid_mask, b_mod, w_mod, sp_size):
    layers, depth, width = w_mod.shape
    tokens = positions.shape[0]
    cols = width // NDEV
    vmem = pl.BlockSpec(memory_space=pltpu.VMEM)
    table = jax.ShapeDtypeStruct((tokens, HEAD), jnp.float32)
    return pl.pallas_call(
        functools.partial(mods_body, sp_size=sp_size),
        out_shape=(jax.ShapeDtypeStruct((8, width), jnp.float32), table, table),
        in_specs=[vmem] * 4 + [pl.BlockSpec(memory_space=pl.ANY)],
        out_specs=(vmem, vmem, vmem),
        scratch_shapes=[
            pltpu.VMEM((layers, depth, cols), jnp.bfloat16),
            pltpu.VMEM((8, cols), jnp.float32),
            pltpu.SemaphoreType.DMA((layers, K_CUT)),
            pltpu.SemaphoreType.DMA((NDEV - 1,)),
            pltpu.SemaphoreType.DMA((NDEV - 1,)),
        ],
        compiler_params=pltpu.CompilerParams(collective_id=16, has_side_effects=True),
        cost_estimate=pl.CostEstimate(flops=32 * layers * depth * cols, bytes_accessed=2 * layers * depth * cols, transcendentals=2 * tokens * HEAD),
        name='mods',
    )(cond_vec, positions, valid_mask, b_mod, w_mod)


QW = 512
MW = 1024
QH = QW // HEAD


def front_body(x_ref, mods_ref, b_ref, bo_ref, qg_ref, kg_ref, cos_ref, sin_ref, w_in_ref, w_out_ref,
               recv_ref, y_hbm, h_ref, y_ref, win_ref, wout_ref, send_ref, act_ref,
               in_sem, out_sem, y_sem, send_sem, recv_sem, keep_sem, *, layer, sp_size):
    tokens, dim = x_ref.shape
    q_steps = dim // QW
    mlp_dim = w_out_ref.shape[1] - dim
    m_steps = mlp_dim // MW
    me = lax.axis_index('cp') * sp_size + lax.axis_index('sp')
    halves = NDEV // QH

    def in_copy(col, slot, idx):
        return pltpu.make_async_copy(w_in_ref.at[layer, :, pl.ds(pl.multiple_of(col, QW), QW)], win_ref.at[slot, idx], in_sem.at[slot, idx])

    def out_copy(step, slot):
        return pltpu.make_async_copy(w_out_ref.at[layer, pl.ds(pl.multiple_of(dim + step * MW, MW), MW), :], wout_ref.at[slot], out_sem.at[slot])

    def q_cols(step):
        return [w * dim + step * QW for w in range(3)]

    def m_cols(step):
        return [3 * dim + step * MW + i * QW for i in range(MW // QW)]

    def landing(part):
        return recv_ref.at[part, :, pl.ds(pl.multiple_of(me * tokens, tokens), tokens), :]

    def keep(part):
        return pltpu.make_async_copy(send_ref.at[part * NDEV + me], landing(part), keep_sem.at[part])

    def send(step):
        part = step // halves
        for dd in range(QH):
            dest = (step % halves) * QH + dd

            @pl.when(dest != me)
            def _():
                pltpu.make_async_remote_copy(
                    src_ref=send_ref.at[part * NDEV + dest], dst_ref=landing(part),
                    send_sem=send_sem, recv_sem=recv_sem,
                    device_id=device_of(dest, sp_size), device_id_type=pl.DeviceIdType.MESH).start()

            @pl.when(dest == me)
            def _():
                keep(part).start()

    for w, col in enumerate(q_cols(0)):
        in_copy(col, 0, w).start()
    barrier = meet_all(me, sp_size)

    rows = 16
    shift = mods_ref[layer:layer + 1, :dim]
    scale_p = 1.0 + mods_ref[layer:layer + 1, dim:2 * dim]
    bias_out = jnp.broadcast_to(bo_ref[...].astype(jnp.float32)[layer:layer + 1], (rows, dim))
    gains = [g_ref[...].astype(jnp.float32)[layer:layer + 1] for g_ref in (qg_ref, kg_ref)]

    def norm_rows(r, carry):
        at = pl.ds(pl.multiple_of(r * rows, rows), rows)
        v = x_ref[at, :].astype(jnp.float32)
        v = v - jnp.mean(v, axis=-1, keepdims=True)
        var = jnp.mean(v * v, axis=-1, keepdims=True)
        h_ref[at, :] = (v * lax.rsqrt(var + EPS) * scale_p + shift).astype(jnp.bfloat16)
        y_ref[at, :] = bias_out
        return carry

    lax.fori_loop(0, tokens // rows, norm_rows, 0)

    even = lax.broadcasted_iota(jnp.int32, (1, HEAD), 1) % 2 == 0

    def project(slot, idx, col):
        acc = jnp.dot(h_ref[...], win_ref[slot, idx], preferred_element_type=jnp.float32)
        bias = b_ref[:, pl.ds(pl.multiple_of(col, QW), QW)].astype(jnp.float32)[layer:layer + 1]
        return (acc + bias).astype(jnp.bfloat16)

    def q_step(t, carry):
        slot = t % 2
        for w, col in enumerate(q_cols(t)):
            in_copy(col, slot, w).wait()

        @pl.when(t + 1 < q_steps)
        def _():
            for w, col in enumerate(q_cols(t + 1)):
                in_copy(col, 1 - slot, w).start()

        @pl.when(t + 1 == q_steps)
        def _():
            for i, col in enumerate(m_cols(0)):
                in_copy(col, 1 - slot, i).start()
            out_copy(0, 1 - slot).start()

        @pl.when(t == 1)
        def _():
            pl.semaphore_wait(barrier, NDEV - 1)

        @pl.when(t > 0)
        def _():
            send(t - 1)

        for w, col in enumerate(q_cols(t)):
            u = project(slot, w, col)
            for n in range(QH):
                piece = u[:, n * HEAD:(n + 1) * HEAD]
                if w < 2:
                    v = piece.astype(jnp.float32)
                    v = v * lax.rsqrt(jnp.mean(v * v, axis=-1, keepdims=True) + EPS) * gains[w]
                    swapped = jnp.where(even, pltpu.roll(v, HEAD - 1, 1), pltpu.roll(v, 1, 1))
                    piece = (v * cos_ref[...] + swapped * sin_ref[...]).astype(jnp.bfloat16)
                send_ref[t * QH + n, w] = piece
        return carry

    lax.fori_loop(0, q_steps, q_step, 0)

    def m_step(b, carry):
        slot = (q_steps + b) % 2
        for i, col in enumerate(m_cols(b)):
            in_copy(col, slot, i).wait()
        out_copy(b, slot).wait()

        @pl.when(b + 1 < m_steps)
        def _():
            for i, col in enumerate(m_cols(b + 1)):
                in_copy(col, 1 - slot, i).start()
            out_copy(b + 1, 1 - slot).start()

        @pl.when(b == 0)
        def _():
            send(q_steps - 1)

        for i, col in enumerate(m_cols(b)):
            v = project(slot, i, col).astype(jnp.float32)
            inner = v * (0.7978845608028654 + (0.7978845608028654 * 0.044715) * (v * v))
            half = 0.5 * v
            act_ref[i] = (half + half * jnp.tanh(inner)).astype(jnp.bfloat16)
        for i in range(MW // QW):
            y_ref[...] += jnp.dot(act_ref[i], wout_ref[slot, i * QW:(i + 1) * QW, :], preferred_element_type=jnp.float32)
        return carry

    lax.fori_loop(0, m_steps, m_step, 0)
    y_copy = pltpu.make_async_copy(y_ref, y_hbm, y_sem)
    y_copy.start()
    parts = q_steps // halves
    moved = send_ref.at[pl.ds(0, parts * (NDEV - 1))]
    pltpu.make_async_copy(moved, moved, send_sem).wait()
    pltpu.make_async_copy(moved, moved, recv_sem).wait()
    for part in range(parts):
        keep(part).wait()
    y_copy.wait()


def front(state, mods, b_in, b_out, q_gain, k_gain, cos_t, sin_t, w_in, w_out, layer, sp_size):
    tokens, dim = state.shape
    mlp_dim = w_out.shape[1] - dim
    vmem = pl.BlockSpec(memory_space=pltpu.VMEM)
    hbm = pl.BlockSpec(memory_space=pl.ANY)
    parts = dim // (NDEV * HEAD)
    flops = 2 * tokens * dim * (3 * dim + 2 * mlp_dim)
    return pl.pallas_call(
        functools.partial(front_body, layer=layer, sp_size=sp_size),
        out_shape=(jax.ShapeDtypeStruct((parts, 3, NDEV * tokens, HEAD), jnp.bfloat16),
                   jax.ShapeDtypeStruct((tokens, dim), jnp.float32)),
        in_specs=[vmem] * 8 + [hbm, hbm],
        out_specs=(hbm, hbm),
        scratch_shapes=[
            pltpu.VMEM((tokens, dim), jnp.bfloat16),
            pltpu.VMEM((tokens, dim), jnp.float32),
            pltpu.VMEM((2, 3, dim, QW), jnp.bfloat16),
            pltpu.VMEM((2, MW, dim), jnp.bfloat16),
            pltpu.VMEM((parts * NDEV, 3, tokens, HEAD), jnp.bfloat16),
            pltpu.VMEM((MW // QW, tokens, QW), jnp.bfloat16),
            pltpu.SemaphoreType.DMA((2, 3)),
            pltpu.SemaphoreType.DMA((2,)),
            pltpu.SemaphoreType.DMA,
            pltpu.SemaphoreType.DMA,
            pltpu.SemaphoreType.DMA,
            pltpu.SemaphoreType.DMA((parts,)),
        ],
        compiler_params=pltpu.CompilerParams(collective_id=layer, has_side_effects=True, vmem_limit_bytes=62 * 1024 * 1024),
        cost_estimate=pl.CostEstimate(flops=flops, bytes_accessed=2 * dim * (3 * dim + 2 * mlp_dim), transcendentals=tokens * mlp_dim),
        name=f'front{layer}',
    )(state, mods, b_in, b_out, q_gain, k_gain, cos_t, sin_t, w_in, w_out)


KC = 768
SUBS = 1


def back_body(recv_ref, mods_ref, x_hbm, y_hbm, w_hbm, o_ref,
              kv_ref, vt_ref, qt_ref, s_ref, p_ref, mask_ref, send_ref, a_ref, x_ref, y_ref, w_ref,
              kv_sem, load_sem, send_sem, recv_sem, keep_sem, *, layer, sp_size):
    tokens, dim = o_ref.shape
    parts, _, seq, _ = recv_ref.shape
    me = lax.axis_index('cp') * sp_size + lax.axis_index('sp')
    chips = NDEV // 2
    q_rows = seq // chips
    turns = chips // SUBS
    steps = parts * turns
    factor = (HEAD ** -0.5) * LOG2E

    def kv_copy(part, slot):
        return pltpu.make_async_copy(recv_ref.at[part], kv_ref.at[slot], kv_sem.at[slot])

    loads = [
        pltpu.make_async_copy(w_hbm.at[layer, pl.ds(0, dim), :], w_ref, load_sem.at[0]),
        pltpu.make_async_copy(y_hbm, y_ref, load_sem.at[1]),
        pltpu.make_async_copy(x_hbm, x_ref, load_sem.at[2]),
    ]
    kv_copy(0, 0).start()
    barrier = meet_all(me, sp_size)
    mask_at = (NDEV - 1) * (mods_ref.shape[1] // NDEV)
    mask_ref[...] = jnp.broadcast_to(mods_ref[MASK_ROW:MASK_ROW + 1, mask_at:mask_at + tokens], (HEAD, tokens)).T

    def chip_at(t, sub):
        return (me // 2 + 1 + t % turns * SUBS + sub) % chips

    def landing(part):
        return a_ref.at[:, pl.ds(pl.multiple_of((part * NDEV + me) * HEAD, HEAD), HEAD)]

    def keep(part):
        return pltpu.make_async_copy(send_ref.at[part * NDEV + me], landing(part), keep_sem.at[part])

    def send(t):
        part = t // turns
        for sub in range(SUBS):
            for core in range(2):
                dest = chip_at(t, sub) * 2 + core

                @pl.when(dest != me)
                def _():
                    pltpu.make_async_remote_copy(
                        src_ref=send_ref.at[part * NDEV + dest], dst_ref=landing(part),
                        send_sem=send_sem, recv_sem=recv_sem.at[part],
                        device_id=device_of(dest, sp_size), device_id_type=pl.DeviceIdType.MESH).start()

                @pl.when(dest == me)
                def _():
                    keep(part).start()

    def attend(t, carry):
        part = t // turns
        slot = part % 2

        @pl.when(t % turns == 0)
        def _():
            kv_copy(part, slot).wait()

            @pl.when(part + 1 < parts)
            def _():
                kv_copy(part + 1, 1 - slot).start()

            for c in range(seq // KC):
                vt_ref[:, c * KC:(c + 1) * KC] = kv_ref[slot, 2, c * KC:(c + 1) * KC, :].T

        @pl.when(t == 1)
        def _():
            pl.semaphore_wait(barrier, NDEV - 1)

        @pl.when(t > 0)
        def _():
            send(t - 1)

        blocks = seq // KC
        items = [(sub, c) for sub in range(SUBS) for c in range(blocks)]
        maxes = {sub: [jnp.full((1, q_rows), -1e30, jnp.float32)] for sub in range(SUBS)}
        total = acc = None

        def scores(i):
            sub, c = items[i]
            if c == 0:
                chip = chip_at(t, sub)
                qt_ref[sub] = kv_ref[slot, 0, pl.ds(pl.multiple_of(chip * q_rows, q_rows), q_rows), :].T
            s = jnp.dot(kv_ref[slot, 1, c * KC:(c + 1) * KC, :], qt_ref[sub], preferred_element_type=jnp.float32)
            if c + 1 == blocks:
                valid = jnp.concatenate([mask_ref[...]] * (q_rows // HEAD), axis=1) > 0
                s = jnp.concatenate([s[:KC - tokens], jnp.where(valid, s[KC - tokens:], -1e30)], axis=0)
            s_ref[i % 2] = s
            maxes[sub].append(jnp.maximum(maxes[sub][-1], jnp.max(s, axis=0, keepdims=True)))

        scores(0)
        for i, (sub, c) in enumerate(items):
            if i + 1 < len(items):
                scores(i + 1)
            p = jnp.exp2((s_ref[i % 2] - maxes[sub][c + 1]) * factor)
            row = jnp.sum(p, axis=0, keepdims=True)
            p_ref[i % 2] = p.astype(jnp.bfloat16)
            pv = jnp.dot(vt_ref[:, c * KC:(c + 1) * KC], p_ref[i % 2], preferred_element_type=jnp.float32)
            if c == 0:
                total, acc = row, pv
            else:
                alpha = jnp.exp2((maxes[sub][c] - maxes[sub][c + 1]) * factor)
                total, acc = total * alpha + row, acc * alpha + pv
            if c + 1 == blocks:
                out = (acc * (1.0 / total)).astype(jnp.bfloat16).T
                for core in range(2):
                    send_ref[part * NDEV + chip_at(t, sub) * 2 + core] = out[core * tokens:(core + 1) * tokens]
        return carry

    for load in loads:
        load.start()
    lax.fori_loop(0, steps, attend, 0)
    send(steps - 1)

    def arrived(part):
        moved = send_ref.at[pl.ds(0, NDEV - 1)]
        pltpu.make_async_copy(moved, moved, recv_sem.at[part]).wait()
        keep(part).wait()

    for load in loads:
        load.wait()
    for part in range(parts - 1):
        arrived(part)
    split = (parts - 1) * NDEV * HEAD
    for n in range(0, dim, QW):
        y_ref[:, n:n + QW] += jnp.dot(a_ref[:, :split], w_ref[:split, n:n + QW], preferred_element_type=jnp.float32)
    arrived(parts - 1)
    for n in range(0, dim, QW):
        y = y_ref[:, n:n + QW] + jnp.dot(a_ref[:, split:], w_ref[split:, n:n + QW], preferred_element_type=jnp.float32)
        o_ref[:, n:n + QW] = (x_ref[:, n:n + QW].astype(jnp.float32) + mods_ref[layer:layer + 1, 2 * dim + n:2 * dim + n + QW] * y).astype(jnp.bfloat16)
    moved = send_ref.at[pl.ds(0, parts * (NDEV - 1))]
    pltpu.make_async_copy(moved, moved, send_sem).wait()


def back(recv, mods, state, y_mlp, w_out, layer, sp_size):
    tokens, dim = state.shape
    parts, _, seq, _ = recv.shape
    q_rows = seq // (NDEV // 2)
    vmem = pl.BlockSpec(memory_space=pltpu.VMEM)
    hbm = pl.BlockSpec(memory_space=pl.ANY)
    return pl.pallas_call(
        functools.partial(back_body, layer=layer, sp_size=sp_size),
        out_shape=jax.ShapeDtypeStruct((tokens, dim), jnp.bfloat16),
        in_specs=[hbm, vmem, hbm, hbm, hbm],
        out_specs=vmem,
        scratch_shapes=[
            pltpu.VMEM((2, 3, seq, HEAD), jnp.bfloat16),
            pltpu.VMEM((HEAD, seq), jnp.bfloat16),
            pltpu.VMEM((SUBS, HEAD, q_rows), jnp.bfloat16),
            pltpu.VMEM((2, KC, q_rows), jnp.float32),
            pltpu.VMEM((2, KC, q_rows), jnp.bfloat16),
            pltpu.VMEM((tokens, HEAD), jnp.float32),
            pltpu.VMEM((parts * NDEV, tokens, HEAD), jnp.bfloat16),
            pltpu.VMEM((tokens, dim), jnp.bfloat16),
            pltpu.VMEM((tokens, dim), jnp.bfloat16),
            pltpu.VMEM((tokens, dim), jnp.float32),
            pltpu.VMEM((dim, dim), jnp.bfloat16),
            pltpu.SemaphoreType.DMA((2,)),
            pltpu.SemaphoreType.DMA((3,)),
            pltpu.SemaphoreType.DMA,
            pltpu.SemaphoreType.DMA((parts,)),
            pltpu.SemaphoreType.DMA((parts,)),
        ],
        compiler_params=pltpu.CompilerParams(collective_id=8 + layer, has_side_effects=True, vmem_limit_bytes=62 * 1024 * 1024),
        cost_estimate=pl.CostEstimate(flops=4 * parts * seq * seq * HEAD + 2 * tokens * dim * dim, bytes_accessed=2 * dim * dim, transcendentals=parts * seq * seq),
        name=f'back{layer}',
    )(recv, mods, state, y_mlp, w_out)


def solution(mesh):
    tok_spec = P('part', AXES, None)
    mask_spec = P('part', AXES)
    vec_spec = P('part', None)
    rep = P()

    def local_blocks(hidden, valid_mask, positions, cond_vec, w_mod, b_mod, w_in, b_in, q_gain, k_gain, w_out, b_out):
        sp_size = mesh.shape['sp']
        mods, cos_t, sin_t = modulation(cond_vec, positions[0], valid_mask, b_mod, w_mod, sp_size)
        state = hidden[0]
        for layer in range(w_in.shape[0]):
            recv, y_mlp = front(state, mods, b_in, b_out, q_gain, k_gain, cos_t, sin_t, w_in, w_out, layer, sp_size)
            state = back(recv, mods, state, y_mlp, w_out, layer, sp_size)
        return state[None]

    in_specs = (tok_spec, mask_spec, tok_spec, vec_spec, rep, rep, rep, rep, rep, rep, rep, rep)
    return jax.shard_map(local_blocks, mesh=mesh, in_specs=in_specs, out_specs=tok_spec, check_vma=False)
```

```python
import functools

import jax
import jax.numpy as jnp
from jax import lax
from jax.experimental import pallas as pl
from jax.experimental.pallas import tpu as pltpu
from jax.sharding import PartitionSpec as P

ROPE_SPLIT = (16, 56, 56)
LOG2_THETA = 8.0
EPS = 1e-6
LOG2E = 1.4426950408889634
HEAD = 128
NDEV = 8
AXES = ('cp', 'sp')


def device_of(index, sp_size):
    return {'part': lax.axis_index('part'), 'cp': index // sp_size, 'sp': index % sp_size}


def meet_all(me, sp_size):
    barrier = pltpu.get_barrier_semaphore()
    for k in range(1, NDEV):
        pl.semaphore_signal(barrier, inc=1, device_id=device_of((me + k) % NDEV, sp_size), device_id_type=pl.DeviceIdType.MESH)
    return barrier


MASK_ROW = 2
K_CUT = 3


def mods_body(cond_ref, pos_ref, mask_ref, b_ref, w_hbm, mods_ref, cos_ref, sin_ref, w_ref, stage_ref, w_sem, send_sem, recv_sem, *, sp_size):
    layers, depth, cols = w_ref.shape
    me = lax.axis_index('cp') * sp_size + lax.axis_index('sp')
    mine = pl.ds(pl.multiple_of(me * cols, HEAD), cols)
    cut = depth // K_CUT

    def w_copy(layer, k):
        rows = pl.ds(k * cut, cut)
        return pltpu.make_async_copy(w_hbm.at[layer, rows, mine], w_ref.at[layer, rows, :], w_sem.at[layer, k])

    for layer in range(layers):
        for k in range(K_CUT):
            w_copy(layer, k).start()
    barrier = meet_all(me, sp_size)

    lane = lax.broadcasted_iota(jnp.int32, (1, HEAD), 1)
    angles = None
    start = 0
    for axis_idx, width in enumerate(ROPE_SPLIT):
        pair = ((lane - start) // 2).astype(jnp.float32)
        freq = jnp.exp2(pair * (-2.0 * LOG2_THETA / width))
        freq = jnp.where((lane >= start) & (lane < start + width), freq, 0.0)
        term = pos_ref[:, axis_idx:axis_idx + 1].astype(jnp.float32) * freq
        angles = term if angles is None else angles + term
        start += width
    cos_ref[...] = jnp.cos(angles)
    sine = jnp.sin(angles)
    sin_ref[...] = jnp.where(lane % 2 == 0, -sine, sine)

    cond = cond_ref[...]
    c_vec = jnp.broadcast_to(cond * jax.nn.sigmoid(cond), (16, depth)).astype(jnp.bfloat16)
    stage_ref[...] = jnp.zeros_like(stage_ref)
    stage_ref[MASK_ROW:MASK_ROW + 1, :mask_ref.shape[1]] = mask_ref[...].astype(jnp.float32)
    for layer in range(layers):
        acc = None
        for k in range(K_CUT):
            w_copy(layer, k).wait()
            part = jnp.dot(c_vec[:, k * cut:(k + 1) * cut], w_ref[layer, k * cut:(k + 1) * cut, :], preferred_element_type=jnp.float32)
            acc = part if acc is None else acc + part
        stage_ref[layer:layer + 1, :] = acc[0:1] + b_ref[:, mine].astype(jnp.float32)[layer:layer + 1]
    mods_ref[:, mine] = stage_ref[...]
    pl.semaphore_wait(barrier, NDEV - 1)
    sends = [
        pltpu.make_async_remote_copy(
            src_ref=stage_ref, dst_ref=mods_ref.at[:, mine], send_sem=send_sem.at[k - 1], recv_sem=recv_sem.at[k - 1],
            device_id=device_of((me + k) % NDEV, sp_size), device_id_type=pl.DeviceIdType.MESH)
        for k in range(1, NDEV)
    ]
    for copy in sends:
        copy.start()
    for copy in sends:
        copy.wait()


def modulation(cond_vec, positions, valid_mask, b_mod, w_mod, sp_size):
    layers, depth, width = w_mod.shape
    tokens = positions.shape[0]
    cols = width // NDEV
    vmem = pl.BlockSpec(memory_space=pltpu.VMEM)
    table = jax.ShapeDtypeStruct((tokens, HEAD), jnp.float32)
    return pl.pallas_call(
        functools.partial(mods_body, sp_size=sp_size),
        out_shape=(jax.ShapeDtypeStruct((8, width), jnp.float32), table, table),
        in_specs=[vmem] * 4 + [pl.BlockSpec(memory_space=pl.ANY)],
        out_specs=(vmem, vmem, vmem),
        scratch_shapes=[
            pltpu.VMEM((layers, depth, cols), jnp.bfloat16),
            pltpu.VMEM((8, cols), jnp.float32),
            pltpu.SemaphoreType.DMA((layers, K_CUT)),
            pltpu.SemaphoreType.DMA((NDEV - 1,)),
            pltpu.SemaphoreType.DMA((NDEV - 1,)),
        ],
        compiler_params=pltpu.CompilerParams(collective_id=16, has_side_effects=True),
        cost_estimate=pl.CostEstimate(flops=32 * layers * depth * cols, bytes_accessed=2 * layers * depth * cols, transcendentals=2 * tokens * HEAD),
        name='mods',
    )(cond_vec, positions, valid_mask, b_mod, w_mod)


QW = 512
MW = 1024
QH = QW // HEAD
KC = 768


def blocks_body(x_hbm, mods_ref, b_ref, bo_ref, qg_ref, kg_ref, cos_ref, sin_ref, w_in_ref, w_out_ref,
                o_hbm, recv_ref, h_ref, x_ref, y_ref, win_ref, wout_ref, send_ref, act_ref,
                kv_ref, s_ref, mask_ref, a_ref,
                in_sem, out_sem, io_sem, kv_sem, qs_sem, qr_sem, qk_sem, as_sem, ar_sem, ak_sem, *, sp_size):
    tokens, dim = x_ref.shape
    layers = w_in_ref.shape[0]
    parts, _, seq, _ = recv_ref.shape[1:]
    me = lax.axis_index('cp') * sp_size + lax.axis_index('sp')
    q_steps = dim // QW
    m_steps = (w_out_ref.shape[1] - dim) // MW
    halves = NDEV // QH
    chips = NDEV // 2
    q_rows = seq // chips
    n_keys = seq // KC
    kinds = 3
    factor = (HEAD ** -0.5) * LOG2E
    vt_ref = wout_ref.at[0, KC:KC + HEAD, :]
    qt_ref = wout_ref.at[1, KC:KC + HEAD, :q_rows]
    even = lax.broadcasted_iota(jnp.int32, (1, HEAD), 1) % 2 == 0
    moved = send_ref.at[pl.ds(0, NDEV - 1)]
    moved_head = send_ref.at[pl.ds(0, NDEV - 1), 0]

    def in_copy(layer, col, slot, idx):
        return pltpu.make_async_copy(w_in_ref.at[layer, :, pl.ds(pl.multiple_of(col, QW), QW)], win_ref.at[slot, idx], in_sem.at[slot, idx])

    def out_copy(layer, step, slot):
        return pltpu.make_async_copy(w_out_ref.at[layer, pl.ds(pl.multiple_of(dim + step * MW, MW), MW), :], wout_ref.at[slot], out_sem.at[slot])

    def attn_w_copy(layer, n):
        return pltpu.make_async_copy(w_out_ref.at[layer, pl.ds(0, dim), pl.ds(n * QW, QW)], win_ref.at[n // kinds, n % kinds], in_sem.at[n // kinds, n % kinds])

    def q_cols(step):
        return [w * dim + step * QW for w in range(kinds)]

    def m_cols(step):
        return [kinds * dim + step * MW + i * QW for i in range(MW // QW)]

    x_in = pltpu.make_async_copy(x_hbm, x_ref, io_sem)
    x_in.start()
    for w, col in enumerate(q_cols(0)):
        in_copy(0, col, 0, w).start()
    barrier = meet_all(me, sp_size)
    mask_at = (NDEV - 1) * (mods_ref.shape[1] // NDEV)
    mask_ref[...] = jnp.broadcast_to(mods_ref[MASK_ROW:MASK_ROW + 1, mask_at:mask_at + tokens], (HEAD, tokens)).T
    x_in.wait()

    for layer in range(layers):

        def q_landing(part, layer=layer):
            return recv_ref.at[layer, part, :, pl.ds(pl.multiple_of(me * tokens, tokens), tokens), :]

        def q_keep(part, layer=layer):
            return pltpu.make_async_copy(send_ref.at[part * NDEV + me], q_landing(part), qk_sem.at[layer, part])

        def q_send(step, layer=layer):
            part = step // halves
            for dd in range(QH):
                dest = (step % halves) * QH + dd

                @pl.when(dest != me)
                def _():
                    pltpu.make_async_remote_copy(
                        src_ref=send_ref.at[part * NDEV + dest], dst_ref=q_landing(part),
                        send_sem=qs_sem.at[layer, part], recv_sem=qr_sem.at[layer, part],
                        device_id=device_of(dest, sp_size), device_id_type=pl.DeviceIdType.MESH).start()

                @pl.when(dest == me)
                def _():
                    q_keep(part).start()

        def q_arrived(part, layer=layer):
            pltpu.make_async_copy(moved, moved, qr_sem.at[layer, part]).wait()
            q_keep(part).wait()

        def q_sent(part, layer=layer):
            pltpu.make_async_copy(moved, moved, qs_sem.at[layer, part]).wait()

        rows = 16
        shift = mods_ref[layer:layer + 1, :dim]
        scale_p = 1.0 + mods_ref[layer:layer + 1, dim:2 * dim]
        bias_out = jnp.broadcast_to(bo_ref[...].astype(jnp.float32)[layer:layer + 1], (rows, dim))
        gains = [g_ref[...].astype(jnp.float32)[layer:layer + 1] for g_ref in (qg_ref, kg_ref)]

        def norm_rows(r, carry):
            at = pl.ds(pl.multiple_of(r * rows, rows), rows)
            v = x_ref[at, :].astype(jnp.float32)
            v = v - jnp.mean(v, axis=-1, keepdims=True)
            var = jnp.mean(v * v, axis=-1, keepdims=True)
            h_ref[at, :] = (v * lax.rsqrt(var + EPS) * scale_p + shift).astype(jnp.bfloat16)
            y_ref[at, :] = bias_out
            return carry

        lax.fori_loop(0, tokens // rows, norm_rows, 0)

        def project(slot, idx, col, layer=layer):
            acc = jnp.dot(h_ref[...], win_ref[slot, idx], preferred_element_type=jnp.float32)
            bias = b_ref[:, pl.ds(pl.multiple_of(col, QW), QW)].astype(jnp.float32)[layer:layer + 1]
            return (acc + bias).astype(jnp.bfloat16)

        def q_step(t, carry, layer=layer):
            slot = t % 2
            for w, col in enumerate(q_cols(t)):
                in_copy(layer, col, slot, w).wait()

            @pl.when(t + 1 < q_steps)
            def _():
                for w, col in enumerate(q_cols(t + 1)):
                    in_copy(layer, col, 1 - slot, w).start()

            @pl.when(t + 1 == q_steps)
            def _():
                for i, col in enumerate(m_cols(0)):
                    in_copy(layer, col, 1 - slot, i).start()
                out_copy(layer, 0, 1 - slot).start()

            if layer == 0:
                @pl.when(t == 1)
                def _():
                    pl.semaphore_wait(barrier, NDEV - 1)

            @pl.when(t > 0)
            def _():
                q_send(t - 1)

            for w, col in enumerate(q_cols(t)):
                u = project(slot, w, col)
                for n in range(QH):
                    piece = u[:, n * HEAD:(n + 1) * HEAD]
                    if w < 2:
                        v = piece.astype(jnp.float32)
                        v = v * lax.rsqrt(jnp.mean(v * v, axis=-1, keepdims=True) + EPS) * gains[w]
                        swapped = jnp.where(even, pltpu.roll(v, HEAD - 1, 1), pltpu.roll(v, 1, 1))
                        piece = (v * cos_ref[...] + swapped * sin_ref[...]).astype(jnp.bfloat16)
                    send_ref[t * QH + n, w] = piece
            return carry

        lax.fori_loop(0, q_steps, q_step, 0)

        def kv_copy(part, slot, layer=layer):
            return pltpu.make_async_copy(recv_ref.at[layer, part], kv_ref.at[slot], kv_sem.at[slot])

        def m_step(b, carry, layer=layer):
            slot = (q_steps + b) % 2
            for i, col in enumerate(m_cols(b)):
                in_copy(layer, col, slot, i).wait()
            out_copy(layer, b, slot).wait()

            @pl.when(b + 1 < m_steps)
            def _():
                for i, col in enumerate(m_cols(b + 1)):
                    in_copy(layer, col, 1 - slot, i).start()
                out_copy(layer, b + 1, 1 - slot).start()

            @pl.when(b == 0)
            def _():
                q_send(q_steps - 1)

            @pl.when(b == m_steps - 1)
            def _():
                q_arrived(0)
                kv_copy(0, 0).start()

            for i, col in enumerate(m_cols(b)):
                v = project(slot, i, col).astype(jnp.float32)
                inner = v * (0.7978845608028654 + (0.7978845608028654 * 0.044715) * (v * v))
                half = 0.5 * v
                act_ref[i] = (half + half * jnp.tanh(inner)).astype(jnp.bfloat16)
            for i in range(MW // QW):
                y_ref[...] += jnp.dot(act_ref[i], wout_ref[slot, i * QW:(i + 1) * QW, :], preferred_element_type=jnp.float32)
            return carry

        lax.fori_loop(0, m_steps, m_step, 0)
        for n in range(q_steps):
            attn_w_copy(layer, n).start()

        def chip_at(t):
            return (me // 2 + 1 + t % chips) % chips

        def a_source(part, dest):
            return send_ref.at[part * NDEV + dest, 0]

        def a_landing(part):
            return a_ref.at[:, pl.ds(pl.multiple_of((part * NDEV + me) * HEAD, HEAD), HEAD)]

        def a_keep(part, layer=layer):
            return pltpu.make_async_copy(a_source(part, me), a_landing(part), ak_sem.at[layer, part])

        def a_send(t, layer=layer):
            part = t // chips
            for core in range(2):
                dest = chip_at(t) * 2 + core

                @pl.when(dest != me)
                def _():
                    pltpu.make_async_remote_copy(
                        src_ref=a_source(part, dest), dst_ref=a_landing(part),
                        send_sem=as_sem.at[layer, part], recv_sem=ar_sem.at[layer, part],
                        device_id=device_of(dest, sp_size), device_id_type=pl.DeviceIdType.MESH).start()

                @pl.when(dest == me)
                def _():
                    a_keep(part).start()

        def a_arrived(part, layer=layer):
            pltpu.make_async_copy(moved_head, moved_head, ar_sem.at[layer, part]).wait()
            a_keep(part).wait()

        def attend(t, carry):
            part = t // chips
            slot = part % 2
            chip = chip_at(t)

            @pl.when(t > 0)
            def _():
                a_send(t - 1)

            @pl.when(t % chips == 0)
            def _():
                q_sent(part)
                kv_copy(part, slot).wait()

                @pl.when(part + 1 < parts)
                def _():
                    q_arrived(part + 1)
                    kv_copy(part + 1, 1 - slot).start()

                for c in range(n_keys):
                    vt_ref[:, c * KC:(c + 1) * KC] = kv_ref[slot, 2, c * KC:(c + 1) * KC, :].T

            qt_ref[...] = kv_ref[slot, 0, pl.ds(pl.multiple_of(chip * q_rows, q_rows), q_rows), :].T
            maxes = [jnp.full((1, q_rows), -1e30, jnp.float32)]

            def scores(c):
                s = jnp.dot(kv_ref[slot, 1, c * KC:(c + 1) * KC, :], qt_ref[...], preferred_element_type=jnp.float32)
                if c + 1 == n_keys:
                    valid = jnp.concatenate([mask_ref[...]] * (q_rows // HEAD), axis=1) > 0
                    s = jnp.concatenate([s[:KC - tokens], jnp.where(valid, s[KC - tokens:], -1e30)], axis=0)
                s_ref[c % 2] = s
                maxes.append(jnp.maximum(maxes[-1], jnp.max(s, axis=0, keepdims=True)))

            total = acc = None
            scores(0)
            for c in range(n_keys):
                if c + 1 < n_keys:
                    scores(c + 1)
                p = jnp.exp2((s_ref[c % 2] - maxes[c + 1]) * factor)
                row = jnp.sum(p, axis=0, keepdims=True)
                wout_ref[c % 2, :KC, :q_rows] = p.astype(jnp.bfloat16)
                pv = jnp.dot(vt_ref[:, c * KC:(c + 1) * KC], wout_ref[c % 2, :KC, :q_rows], preferred_element_type=jnp.float32)
                if c == 0:
                    total, acc = row, pv
                else:
                    alpha = jnp.exp2((maxes[c] - maxes[c + 1]) * factor)
                    total, acc = total * alpha + row, acc * alpha + pv
            out = (acc * (1.0 / total)).astype(jnp.bfloat16).T
            for core in range(2):
                send_ref[part * NDEV + chip * 2 + core, 0] = out[core * tokens:(core + 1) * tokens]
            return carry

        lax.fori_loop(0, parts * chips, attend, 0)
        a_send(parts * chips - 1)

        for n in range(q_steps):
            attn_w_copy(layer, n).wait()
        for part in range(parts - 1):
            a_arrived(part)
        split = (parts - 1) * NDEV * HEAD

        def attn_w(n, cut):
            return win_ref[n // kinds, n % kinds, cut, :]

        for n in range(q_steps):
            cols = slice(n * QW, (n + 1) * QW)
            y_ref[:, cols] += jnp.dot(a_ref[:, :split], attn_w(n, slice(0, split)), preferred_element_type=jnp.float32)
        a_arrived(parts - 1)
        for n in range(q_steps):
            cols = slice(n * QW, (n + 1) * QW)
            y = y_ref[:, cols] + jnp.dot(a_ref[:, split:], attn_w(n, slice(split, dim)), preferred_element_type=jnp.float32)
            gate = mods_ref[layer:layer + 1, 2 * dim + n * QW:2 * dim + (n + 1) * QW]
            x_ref[:, cols] = (x_ref[:, cols].astype(jnp.float32) + gate * y).astype(jnp.bfloat16)
            if n + 1 == kinds and layer + 1 < layers:
                for w, col in enumerate(q_cols(0)):
                    in_copy(layer + 1, col, 0, w).start()
        for part in range(parts):
            pltpu.make_async_copy(moved_head, moved_head, as_sem.at[layer, part]).wait()

    x_out = pltpu.make_async_copy(x_ref, o_hbm, io_sem)
    x_out.start()
    x_out.wait()


def blocks(state, mods, b_in, b_out, q_gain, k_gain, cos_t, sin_t, w_in, w_out, sp_size):
    tokens, dim = state.shape
    layers = w_in.shape[0]
    mlp_dim = w_out.shape[1] - dim
    parts = dim // (NDEV * HEAD)
    seq = NDEV * tokens
    q_rows = seq // (NDEV // 2)
    vmem = pl.BlockSpec(memory_space=pltpu.VMEM)
    hbm = pl.BlockSpec(memory_space=pl.ANY)
    dma = pltpu.SemaphoreType.DMA
    flops = layers * (2 * tokens * dim * (4 * dim + 2 * mlp_dim) + 4 * parts * seq * seq * HEAD)
    out, _ = pl.pallas_call(
        functools.partial(blocks_body, sp_size=sp_size),
        out_shape=(jax.ShapeDtypeStruct((tokens, dim), jnp.bfloat16),
                   jax.ShapeDtypeStruct((layers, parts, 3, seq, HEAD), jnp.bfloat16)),
        in_specs=[hbm] + [vmem] * 7 + [hbm, hbm],
        out_specs=(hbm, hbm),
        scratch_shapes=[
            pltpu.VMEM((tokens, dim), jnp.bfloat16),
            pltpu.VMEM((tokens, dim), jnp.bfloat16),
            pltpu.VMEM((tokens, dim), jnp.float32),
            pltpu.VMEM((2, 3, dim, QW), jnp.bfloat16),
            pltpu.VMEM((2, MW, dim), jnp.bfloat16),
            pltpu.VMEM((parts * NDEV, 3, tokens, HEAD), jnp.bfloat16),
            pltpu.VMEM((MW // QW, tokens, QW), jnp.bfloat16),
            pltpu.VMEM((2, 3, seq, HEAD), jnp.bfloat16),
            pltpu.VMEM((2, KC, q_rows), jnp.float32),
            pltpu.VMEM((tokens, HEAD), jnp.float32),
            pltpu.VMEM((tokens, dim), jnp.bfloat16),
            dma((2, 3)), dma((2,)), dma, dma((2,)),
            dma((layers, parts)), dma((layers, parts)), dma((layers, parts)),
            dma((layers, parts)), dma((layers, parts)), dma((layers, parts)),
        ],
        compiler_params=pltpu.CompilerParams(collective_id=0, has_side_effects=True, vmem_limit_bytes=67043328),
        cost_estimate=pl.CostEstimate(flops=flops, bytes_accessed=2 * layers * dim * (4 * dim + 2 * mlp_dim), transcendentals=layers * parts * seq * seq),
        name='blocks',
    )(state, mods, b_in, b_out, q_gain, k_gain, cos_t, sin_t, w_in, w_out)
    return out


def solution(mesh):
    tok_spec = P('part', AXES, None)
    mask_spec = P('part', AXES)
    vec_spec = P('part', None)
    rep = P()

    def local_blocks(hidden, valid_mask, positions, cond_vec, w_mod, b_mod, w_in, b_in, q_gain, k_gain, w_out, b_out):
        sp_size = mesh.shape['sp']
        mods, cos_t, sin_t = modulation(cond_vec, positions[0], valid_mask, b_mod, w_mod, sp_size)
        state = blocks(hidden[0], mods, b_in, b_out, q_gain, k_gain, cos_t, sin_t, w_in, w_out, sp_size)
        return state[None]

    in_specs = (tok_spec, mask_spec, tok_spec, vec_spec, rep, rep, rep, rep, rep, rep, rep, rep)
    return jax.shard_map(local_blocks, mesh=mesh, in_specs=in_specs, out_specs=tok_spec, check_vma=False)
```

```python
import functools

import jax
import jax.numpy as jnp
from jax import lax
from jax.experimental import pallas as pl
from jax.experimental.pallas import tpu as pltpu
from jax.sharding import PartitionSpec as P

ROPE_SPLIT = (16, 56, 56)
LOG2_THETA = 8.0
EPS = 1e-6
LOG2E = 1.4426950408889634
HEAD = 128
NDEV = 8
AXES = ('cp', 'sp')


def device_of(index, sp_size):
    return {'part': lax.axis_index('part'), 'cp': index // sp_size, 'sp': index % sp_size}


def meet_all(me, sp_size):
    barrier = pltpu.get_barrier_semaphore()
    for k in range(1, NDEV):
        pl.semaphore_signal(barrier, inc=1, device_id=device_of((me + k) % NDEV, sp_size), device_id_type=pl.DeviceIdType.MESH)
    return barrier


MASK_ROW = 2
K_CUT = 3


def mods_body(cond_ref, pos_ref, mask_ref, b_ref, w_hbm, mods_ref, cos_ref, sin_ref, w_ref, stage_ref, w_sem, send_sem, recv_sem, *, sp_size):
    layers, depth, cols = w_ref.shape
    me = lax.axis_index('cp') * sp_size + lax.axis_index('sp')
    mine = pl.ds(pl.multiple_of(me * cols, HEAD), cols)
    cut = depth // K_CUT

    def w_copy(layer, k):
        rows = pl.ds(k * cut, cut)
        return pltpu.make_async_copy(w_hbm.at[layer, rows, mine], w_ref.at[layer, rows, :], w_sem.at[layer, k])

    for layer in range(layers):
        for k in range(K_CUT):
            w_copy(layer, k).start()
    barrier = meet_all(me, sp_size)

    lane = lax.broadcasted_iota(jnp.int32, (HEAD, 1), 0)
    angles = None
    start = 0
    for axis_idx, width in enumerate(ROPE_SPLIT):
        pair = ((lane - start) // 2).astype(jnp.float32)
        freq = jnp.exp2(pair * (-2.0 * LOG2_THETA / width))
        freq = jnp.where((lane >= start) & (lane < start + width), freq, 0.0)
        term = pos_ref[axis_idx:axis_idx + 1, :].astype(jnp.float32) * freq
        angles = term if angles is None else angles + term
        start += width
    cos_ref[...] = jnp.cos(angles).T
    sine = jnp.sin(angles)
    sin_ref[...] = jnp.where(lane % 2 == 0, -sine, sine).T

    cond = cond_ref[...]
    c_vec = jnp.broadcast_to(cond * jax.nn.sigmoid(cond), (16, depth)).astype(jnp.bfloat16)
    stage_ref[...] = jnp.zeros_like(stage_ref)
    stage_ref[MASK_ROW:MASK_ROW + 1, :mask_ref.shape[1]] = mask_ref[...].astype(jnp.float32)
    for layer in range(layers):
        acc = None
        for k in range(K_CUT):
            w_copy(layer, k).wait()
            part = jnp.dot(c_vec[:, k * cut:(k + 1) * cut], w_ref[layer, k * cut:(k + 1) * cut, :], preferred_element_type=jnp.float32)
            acc = part if acc is None else acc + part
        stage_ref[layer:layer + 1, :] = acc[0:1] + b_ref[:, mine].astype(jnp.float32)[layer:layer + 1]
    mods_ref[:, mine] = stage_ref[...]
    pl.semaphore_wait(barrier, NDEV - 1)
    sends = [
        pltpu.make_async_remote_copy(
            src_ref=stage_ref, dst_ref=mods_ref.at[:, mine], send_sem=send_sem.at[k - 1], recv_sem=recv_sem.at[k - 1],
            device_id=device_of((me + k) % NDEV, sp_size), device_id_type=pl.DeviceIdType.MESH)
        for k in range(1, NDEV)
    ]
    for copy in sends:
        copy.start()
    for copy in sends:
        copy.wait()


def modulation(cond_vec, positions, valid_mask, b_mod, w_mod, sp_size):
    layers, depth, width = w_mod.shape
    tokens = positions.shape[1]
    cols = width // NDEV
    vmem = pl.BlockSpec(memory_space=pltpu.VMEM)
    table = jax.ShapeDtypeStruct((tokens, HEAD), jnp.float32)
    return pl.pallas_call(
        functools.partial(mods_body, sp_size=sp_size),
        out_shape=(jax.ShapeDtypeStruct((8, width), jnp.float32), table, table),
        in_specs=[vmem] * 4 + [pl.BlockSpec(memory_space=pl.ANY)],
        out_specs=(vmem, vmem, vmem),
        scratch_shapes=[
            pltpu.VMEM((layers, depth, cols), jnp.bfloat16),
            pltpu.VMEM((8, cols), jnp.float32),
            pltpu.SemaphoreType.DMA((layers, K_CUT)),
            pltpu.SemaphoreType.DMA((NDEV - 1,)),
            pltpu.SemaphoreType.DMA((NDEV - 1,)),
        ],
        compiler_params=pltpu.CompilerParams(collective_id=16, has_side_effects=True),
        cost_estimate=pl.CostEstimate(flops=32 * layers * depth * cols, bytes_accessed=2 * layers * depth * cols, transcendentals=2 * tokens * HEAD),
        name='mods',
    )(cond_vec, positions, valid_mask, b_mod, w_mod)


QW = 512
MW = 1024
QH = QW // HEAD
KC = 768


def blocks_body(x_hbm, mods_ref, b_ref, bo_ref, qg_ref, kg_ref, cos_ref, sin_ref, w_in_ref, w_out_ref,
                o_hbm, recv_ref, h_ref, x_ref, y_ref, win_ref, wout_ref, send_ref, act_ref,
                kv_ref, s_ref, mask_ref, a_ref,
                in_sem, out_sem, io_sem, kv_sem, qs_sem, qr_sem, qk_sem, as_sem, ar_sem, ak_sem, *, sp_size):
    tokens, dim = x_ref.shape
    layers = w_in_ref.shape[0]
    parts, _, seq, _ = recv_ref.shape[1:]
    me = lax.axis_index('cp') * sp_size + lax.axis_index('sp')
    q_steps = dim // QW
    m_steps = (w_out_ref.shape[1] - dim) // MW
    halves = NDEV // QH
    chips = NDEV // 2
    q_rows = seq // chips
    n_keys = seq // KC
    kinds = 3
    factor = (HEAD ** -0.5) * LOG2E
    vt_ref = wout_ref.at[0, KC:KC + HEAD, :]
    qt_ref = wout_ref.at[1, KC:KC + HEAD, :q_rows]
    even = lax.broadcasted_iota(jnp.int32, (1, HEAD), 1) % 2 == 0
    moved = send_ref.at[pl.ds(0, NDEV - 1)]
    moved_head = send_ref.at[pl.ds(0, NDEV - 1), 0]

    def in_copy(layer, col, slot, idx):
        return pltpu.make_async_copy(w_in_ref.at[layer, :, pl.ds(pl.multiple_of(col, QW), QW)], win_ref.at[slot, idx], in_sem.at[slot, idx])

    def out_copy(layer, step, slot):
        return pltpu.make_async_copy(w_out_ref.at[layer, pl.ds(pl.multiple_of(dim + step * MW, MW), MW), :], wout_ref.at[slot], out_sem.at[slot])

    def attn_w_copy(layer, n):
        return pltpu.make_async_copy(w_out_ref.at[layer, pl.ds(0, dim), pl.ds(n * QW, QW)], win_ref.at[n // kinds, n % kinds], in_sem.at[n // kinds, n % kinds])

    def q_cols(step):
        return [w * dim + step * QW for w in range(kinds)]

    def m_cols(step):
        return [kinds * dim + step * MW + i * QW for i in range(MW // QW)]

    x_in = pltpu.make_async_copy(x_hbm, x_ref, io_sem)
    x_in.start()
    for w, col in enumerate(q_cols(0)):
        in_copy(0, col, 0, w).start()
    barrier = meet_all(me, sp_size)
    mask_at = (NDEV - 1) * (mods_ref.shape[1] // NDEV)
    mask_ref[...] = jnp.broadcast_to(mods_ref[MASK_ROW:MASK_ROW + 1, mask_at:mask_at + tokens], (HEAD, tokens)).T
    x_in.wait()

    for layer in range(layers):

        def q_landing(part, layer=layer):
            return recv_ref.at[layer, part, :, pl.ds(pl.multiple_of(me * tokens, tokens), tokens), :]

        def q_keep(part, layer=layer):
            return pltpu.make_async_copy(send_ref.at[part * NDEV + me], q_landing(part), qk_sem.at[layer, part])

        def q_send(step, layer=layer):
            part = step // halves
            for dd in range(QH):
                dest = (step % halves) * QH + dd

                @pl.when(dest != me)
                def _():
                    pltpu.make_async_remote_copy(
                        src_ref=send_ref.at[part * NDEV + dest], dst_ref=q_landing(part),
                        send_sem=qs_sem.at[layer, part], recv_sem=qr_sem.at[layer, part],
                        device_id=device_of(dest, sp_size), device_id_type=pl.DeviceIdType.MESH).start()

                @pl.when(dest == me)
                def _():
                    q_keep(part).start()

        def q_arrived(part, layer=layer):
            pltpu.make_async_copy(moved, moved, qr_sem.at[layer, part]).wait()
            q_keep(part).wait()

        def q_sent(part, layer=layer):
            pltpu.make_async_copy(moved, moved, qs_sem.at[layer, part]).wait()

        rows = 16
        shift = mods_ref[layer:layer + 1, :dim]
        scale_p = 1.0 + mods_ref[layer:layer + 1, dim:2 * dim]
        bias_out = jnp.broadcast_to(bo_ref[...].astype(jnp.float32)[layer:layer + 1], (rows, dim))
        gains = [g_ref[...].astype(jnp.float32)[layer:layer + 1] for g_ref in (qg_ref, kg_ref)]

        def norm_rows(r, carry):
            at = pl.ds(pl.multiple_of(r * rows, rows), rows)
            v = x_ref[at, :].astype(jnp.float32)
            v = v - jnp.mean(v, axis=-1, keepdims=True)
            var = jnp.mean(v * v, axis=-1, keepdims=True)
            h_ref[at, :] = (v * lax.rsqrt(var + EPS) * scale_p + shift).astype(jnp.bfloat16)
            y_ref[at, :] = bias_out
            return carry

        lax.fori_loop(0, tokens // rows, norm_rows, 0, unroll=4)

        def project(slot, idx, col, layer=layer):
            acc = jnp.dot(h_ref[...], win_ref[slot, idx], preferred_element_type=jnp.float32)
            bias = b_ref[:, pl.ds(pl.multiple_of(col, QW), QW)].astype(jnp.float32)[layer:layer + 1]
            return (acc + bias).astype(jnp.bfloat16)

        def q_step(t, carry, layer=layer):
            slot = t % 2
            for w, col in enumerate(q_cols(t)):
                in_copy(layer, col, slot, w).wait()

            @pl.when(t + 1 < q_steps)
            def _():
                for w, col in enumerate(q_cols(t + 1)):
                    in_copy(layer, col, 1 - slot, w).start()

            @pl.when(t + 1 == q_steps)
            def _():
                for i, col in enumerate(m_cols(0)):
                    in_copy(layer, col, 1 - slot, i).start()
                out_copy(layer, 0, 1 - slot).start()

            if layer == 0:
                @pl.when(t == 1)
                def _():
                    pl.semaphore_wait(barrier, NDEV - 1)

            @pl.when(t > 0)
            def _():
                q_send(t - 1)

            for w, col in enumerate(q_cols(t)):
                u = project(slot, w, col)
                for n in range(QH):
                    piece = u[:, n * HEAD:(n + 1) * HEAD]
                    if w < 2:
                        v = piece.astype(jnp.float32)
                        v = v * lax.rsqrt(jnp.mean(v * v, axis=-1, keepdims=True) + EPS) * gains[w]
                        swapped = jnp.where(even, pltpu.roll(v, HEAD - 1, 1), pltpu.roll(v, 1, 1))
                        piece = (v * cos_ref[...] + swapped * sin_ref[...]).astype(jnp.bfloat16)
                    send_ref[t * QH + n, w] = piece
            return carry

        lax.fori_loop(0, q_steps, q_step, 0)

        def kv_copy(part, slot, layer=layer):
            return pltpu.make_async_copy(recv_ref.at[layer, part], kv_ref.at[slot], kv_sem.at[slot])

        def m_step(b, carry, layer=layer):
            slot = (q_steps + b) % 2
            for i, col in enumerate(m_cols(b)):
                in_copy(layer, col, slot, i).wait()
            out_copy(layer, b, slot).wait()

            @pl.when(b + 1 < m_steps)
            def _():
                for i, col in enumerate(m_cols(b + 1)):
                    in_copy(layer, col, 1 - slot, i).start()
                out_copy(layer, b + 1, 1 - slot).start()

            @pl.when(b == 0)
            def _():
                q_send(q_steps - 1)

            @pl.when(b == m_steps - 1)
            def _():
                q_arrived(0)
                kv_copy(0, 0).start()

            for i, col in enumerate(m_cols(b)):
                v = project(slot, i, col).astype(jnp.float32)
                inner = v * (0.7978845608028654 + (0.7978845608028654 * 0.044715) * (v * v))
                half = 0.5 * v
                act_ref[i] = (half + half * jnp.tanh(inner)).astype(jnp.bfloat16)
            for i in range(MW // QW):
                y_ref[...] += jnp.dot(act_ref[i], wout_ref[slot, i * QW:(i + 1) * QW, :], preferred_element_type=jnp.float32)
            return carry

        lax.fori_loop(0, m_steps, m_step, 0)
        for n in range(q_steps):
            attn_w_copy(layer, n).start()

        def chip_at(t):
            return (me // 2 + 1 + t % chips) % chips

        def a_source(part, dest):
            return send_ref.at[part * NDEV + dest, 0]

        def a_landing(part):
            return a_ref.at[:, pl.ds(pl.multiple_of((part * NDEV + me) * HEAD, HEAD), HEAD)]

        def a_keep(part, layer=layer):
            return pltpu.make_async_copy(a_source(part, me), a_landing(part), ak_sem.at[layer, part])

        def a_send(t, layer=layer):
            part = t // chips
            for core in range(2):
                dest = chip_at(t) * 2 + core

                @pl.when(dest != me)
                def _():
                    pltpu.make_async_remote_copy(
                        src_ref=a_source(part, dest), dst_ref=a_landing(part),
                        send_sem=as_sem.at[layer, part], recv_sem=ar_sem.at[layer, part],
                        device_id=device_of(dest, sp_size), device_id_type=pl.DeviceIdType.MESH).start()

                @pl.when(dest == me)
                def _():
                    a_keep(part).start()

        def a_arrived(part, layer=layer):
            pltpu.make_async_copy(moved_head, moved_head, ar_sem.at[layer, part]).wait()
            a_keep(part).wait()

        def attend(t, carry):
            part = t // chips
            slot = part % 2
            chip = chip_at(t)

            @pl.when(t > 0)
            def _():
                a_send(t - 1)

            @pl.when(t % chips == 0)
            def _():
                q_sent(part)
                kv_copy(part, slot).wait()

                @pl.when(part + 1 < parts)
                def _():
                    q_arrived(part + 1)
                    kv_copy(part + 1, 1 - slot).start()

                for c in range(n_keys):
                    vt_ref[:, c * KC:(c + 1) * KC] = kv_ref[slot, 2, c * KC:(c + 1) * KC, :].T

            qt_ref[...] = kv_ref[slot, 0, pl.ds(pl.multiple_of(chip * q_rows, q_rows), q_rows), :].T
            maxes = [jnp.full((1, q_rows), -1e30, jnp.float32)]

            def scores(c):
                s = jnp.dot(kv_ref[slot, 1, c * KC:(c + 1) * KC, :], qt_ref[...], preferred_element_type=jnp.float32)
                if c + 1 == n_keys:
                    valid = jnp.concatenate([mask_ref[...]] * (q_rows // HEAD), axis=1) > 0
                    s = jnp.concatenate([s[:KC - tokens], jnp.where(valid, s[KC - tokens:], -1e30)], axis=0)
                s_ref[c % 2] = s
                maxes.append(jnp.maximum(maxes[-1], jnp.max(s, axis=0, keepdims=True)))

            total = acc = None
            scores(0)
            for c in range(n_keys):
                if c + 1 < n_keys:
                    scores(c + 1)
                p = jnp.exp2((s_ref[c % 2] - maxes[c + 1]) * factor)
                row = jnp.sum(p, axis=0, keepdims=True)
                wout_ref[c % 2, :KC, :q_rows] = p.astype(jnp.bfloat16)
                pv = jnp.dot(vt_ref[:, c * KC:(c + 1) * KC], wout_ref[c % 2, :KC, :q_rows], preferred_element_type=jnp.float32)
                if c == 0:
                    total, acc = row, pv
                else:
                    alpha = jnp.exp2((maxes[c] - maxes[c + 1]) * factor)
                    total, acc = total * alpha + row, acc * alpha + pv
            out = (acc * (1.0 / total)).astype(jnp.bfloat16).T
            for core in range(2):
                send_ref[part * NDEV + chip * 2 + core, 0] = out[core * tokens:(core + 1) * tokens]
            return carry

        lax.fori_loop(0, parts * chips, attend, 0)
        a_send(parts * chips - 1)

        for n in range(q_steps):
            attn_w_copy(layer, n).wait()
        for part in range(parts - 1):
            a_arrived(part)
        split = (parts - 1) * NDEV * HEAD

        def attn_w(n, cut):
            return win_ref[n // kinds, n % kinds, cut, :]

        for n in range(q_steps):
            cols = slice(n * QW, (n + 1) * QW)
            y_ref[:, cols] += jnp.dot(a_ref[:, :split], attn_w(n, slice(0, split)), preferred_element_type=jnp.float32)
        a_arrived(parts - 1)
        for n in range(q_steps):
            cols = slice(n * QW, (n + 1) * QW)
            y = y_ref[:, cols] + jnp.dot(a_ref[:, split:], attn_w(n, slice(split, dim)), preferred_element_type=jnp.float32)
            gate = mods_ref[layer:layer + 1, 2 * dim + n * QW:2 * dim + (n + 1) * QW]
            x_ref[:, cols] = (x_ref[:, cols].astype(jnp.float32) + gate * y).astype(jnp.bfloat16)
            if n + 1 == kinds and layer + 1 < layers:
                for w, col in enumerate(q_cols(0)):
                    in_copy(layer + 1, col, 0, w).start()
        for part in range(parts):
            pltpu.make_async_copy(moved_head, moved_head, as_sem.at[layer, part]).wait()

    x_out = pltpu.make_async_copy(x_ref, o_hbm, io_sem)
    x_out.start()
    x_out.wait()


def blocks(state, mods, b_in, b_out, q_gain, k_gain, cos_t, sin_t, w_in, w_out, sp_size):
    tokens, dim = state.shape
    layers = w_in.shape[0]
    mlp_dim = w_out.shape[1] - dim
    parts = dim // (NDEV * HEAD)
    seq = NDEV * tokens
    q_rows = seq // (NDEV // 2)
    vmem = pl.BlockSpec(memory_space=pltpu.VMEM)
    hbm = pl.BlockSpec(memory_space=pl.ANY)
    dma = pltpu.SemaphoreType.DMA
    flops = layers * (2 * tokens * dim * (4 * dim + 2 * mlp_dim) + 4 * parts * seq * seq * HEAD)
    out, _ = pl.pallas_call(
        functools.partial(blocks_body, sp_size=sp_size),
        out_shape=(jax.ShapeDtypeStruct((tokens, dim), jnp.bfloat16),
                   jax.ShapeDtypeStruct((layers, parts, 3, seq, HEAD), jnp.bfloat16)),
        in_specs=[hbm] + [vmem] * 7 + [hbm, hbm],
        out_specs=(hbm, hbm),
        scratch_shapes=[
            pltpu.VMEM((tokens, dim), jnp.bfloat16),
            pltpu.VMEM((tokens, dim), jnp.bfloat16),
            pltpu.VMEM((tokens, dim), jnp.float32),
            pltpu.VMEM((2, 3, dim, QW), jnp.bfloat16),
            pltpu.VMEM((2, MW, dim), jnp.bfloat16),
            pltpu.VMEM((parts * NDEV, 3, tokens, HEAD), jnp.bfloat16),
            pltpu.VMEM((MW // QW, tokens, QW), jnp.bfloat16),
            pltpu.VMEM((2, 3, seq, HEAD), jnp.bfloat16),
            pltpu.VMEM((2, KC, q_rows), jnp.float32),
            pltpu.VMEM((tokens, HEAD), jnp.float32),
            pltpu.VMEM((tokens, dim), jnp.bfloat16),
            dma((2, 3)), dma((2,)), dma, dma((2,)),
            dma((layers, parts)), dma((layers, parts)), dma((layers, parts)),
            dma((layers, parts)), dma((layers, parts)), dma((layers, parts)),
        ],
        compiler_params=pltpu.CompilerParams(collective_id=0, has_side_effects=True, vmem_limit_bytes=67043328),
        cost_estimate=pl.CostEstimate(flops=flops, bytes_accessed=2 * layers * dim * (4 * dim + 2 * mlp_dim), transcendentals=layers * parts * seq * seq),
        name='blocks',
    )(state, mods, b_in, b_out, q_gain, k_gain, cos_t, sin_t, w_in, w_out)
    return out


def solution(mesh):
    tok_spec = P('part', AXES, None)
    mask_spec = P('part', AXES)
    vec_spec = P('part', None)
    rep = P()

    def local_blocks(hidden, valid_mask, positions, cond_vec, w_mod, b_mod, w_in, b_in, q_gain, k_gain, w_out, b_out):
        sp_size = mesh.shape['sp']
        mods, cos_t, sin_t = modulation(cond_vec, positions[0].T, valid_mask, b_mod, w_mod, sp_size)
        state = blocks(hidden[0], mods, b_in, b_out, q_gain, k_gain, cos_t, sin_t, w_in, w_out, sp_size)
        return state[None]

    in_specs = (tok_spec, mask_spec, tok_spec, vec_spec, rep, rep, rep, rep, rep, rep, rep, rep)
    return jax.shard_map(local_blocks, mesh=mesh, in_specs=in_specs, out_specs=tok_spec, check_vma=False)
```

```python
import functools

import jax
import jax.numpy as jnp
from jax import lax
from jax.experimental import pallas as pl
from jax.experimental.pallas import tpu as pltpu
from jax.sharding import PartitionSpec as P

ROPE_SPLIT = (16, 56, 56)
LOG2_THETA = 8.0
EPS = 1e-6
LOG2E = 1.4426950408889634
HEAD = 128
NDEV = 8
AXES = ('cp', 'sp')


def device_of(index, sp_size):
    return {'part': lax.axis_index('part'), 'cp': index // sp_size, 'sp': index % sp_size}


def meet_all(me, sp_size):
    barrier = pltpu.get_barrier_semaphore()
    for k in range(1, NDEV):
        pl.semaphore_signal(barrier, inc=1, device_id=device_of((me + k) % NDEV, sp_size), device_id_type=pl.DeviceIdType.MESH)
    return barrier


MASK_ROW = 2
K_CUT = 3


def mods_body(cond_ref, pos_ref, mask_ref, b_ref, w_hbm, mods_ref, cos_ref, sin_ref, w_ref, stage_ref, w_sem, send_sem, recv_sem, *, sp_size):
    layers, depth, cols = w_ref.shape
    me = lax.axis_index('cp') * sp_size + lax.axis_index('sp')
    mine = pl.ds(pl.multiple_of(me * cols, HEAD), cols)
    cut = depth // K_CUT

    def w_copy(layer, k):
        rows = pl.ds(k * cut, cut)
        return pltpu.make_async_copy(w_hbm.at[layer, rows, mine], w_ref.at[layer, rows, :], w_sem.at[layer, k])

    for layer in range(layers):
        for k in range(K_CUT):
            w_copy(layer, k).start()
    barrier = meet_all(me, sp_size)

    cond = cond_ref[...]
    c_vec = jnp.broadcast_to(cond * jax.nn.sigmoid(cond), (16, depth)).astype(jnp.bfloat16)
    stage_ref[...] = jnp.zeros_like(stage_ref)
    stage_ref[MASK_ROW:MASK_ROW + 1, :mask_ref.shape[1]] = mask_ref[...].astype(jnp.float32)
    for layer in range(layers):
        acc = None
        for k in range(K_CUT):
            w_copy(layer, k).wait()
            part = jnp.dot(c_vec[:, k * cut:(k + 1) * cut], w_ref[layer, k * cut:(k + 1) * cut, :], preferred_element_type=jnp.float32)
            acc = part if acc is None else acc + part
        stage_ref[layer:layer + 1, :] = acc[0:1] + b_ref[:, mine].astype(jnp.float32)[layer:layer + 1]
    mods_ref[:, mine] = stage_ref[...]
    pl.semaphore_wait(barrier, NDEV - 1)
    sends = [
        pltpu.make_async_remote_copy(
            src_ref=stage_ref, dst_ref=mods_ref.at[:, mine], send_sem=send_sem.at[k - 1], recv_sem=recv_sem.at[k - 1],
            device_id=device_of((me + k) % NDEV, sp_size), device_id_type=pl.DeviceIdType.MESH)
        for k in range(1, NDEV)
    ]
    for copy in sends:
        copy.start()

    lane = lax.broadcasted_iota(jnp.int32, (HEAD, 1), 0)
    angles = None
    start = 0
    for axis_idx, width in enumerate(ROPE_SPLIT):
        pair = ((lane - start) // 2).astype(jnp.float32)
        freq = jnp.exp2(pair * (-2.0 * LOG2_THETA / width))
        freq = jnp.where((lane >= start) & (lane < start + width), freq, 0.0)
        term = pos_ref[axis_idx:axis_idx + 1, :].astype(jnp.float32) * freq
        angles = term if angles is None else angles + term
        start += width
    cos_ref[...] = jnp.cos(angles).T
    sine = jnp.sin(angles)
    sin_ref[...] = jnp.where(lane % 2 == 0, -sine, sine).T

    for copy in sends:
        copy.wait()


def modulation(cond_vec, positions, valid_mask, b_mod, w_mod, sp_size):
    layers, depth, width = w_mod.shape
    tokens = positions.shape[1]
    cols = width // NDEV
    vmem = pl.BlockSpec(memory_space=pltpu.VMEM)
    table = jax.ShapeDtypeStruct((tokens, HEAD), jnp.float32)
    return pl.pallas_call(
        functools.partial(mods_body, sp_size=sp_size),
        out_shape=(jax.ShapeDtypeStruct((8, width), jnp.float32), table, table),
        in_specs=[vmem] * 4 + [pl.BlockSpec(memory_space=pl.ANY)],
        out_specs=(vmem, vmem, vmem),
        scratch_shapes=[
            pltpu.VMEM((layers, depth, cols), jnp.bfloat16),
            pltpu.VMEM((8, cols), jnp.float32),
            pltpu.SemaphoreType.DMA((layers, K_CUT)),
            pltpu.SemaphoreType.DMA((NDEV - 1,)),
            pltpu.SemaphoreType.DMA((NDEV - 1,)),
        ],
        compiler_params=pltpu.CompilerParams(collective_id=16, has_side_effects=True),
        cost_estimate=pl.CostEstimate(flops=32 * layers * depth * cols, bytes_accessed=2 * layers * depth * cols, transcendentals=2 * tokens * HEAD),
        name='mods',
    )(cond_vec, positions, valid_mask, b_mod, w_mod)


QW = 512
MW = 1024
QH = QW // HEAD
KC = 768


def blocks_body(x_hbm, mods_ref, b_ref, bo_ref, qg_ref, kg_ref, cos_ref, sin_ref, w_in_ref, w_out_ref,
                o_hbm, recv_ref, h_ref, x_ref, y_ref, win_ref, wout_ref, send_ref, act_ref,
                kv_ref, s_ref, mask_ref, a_ref,
                in_sem, out_sem, io_sem, kv_sem, qs_sem, qr_sem, qk_sem, as_sem, ar_sem, ak_sem, *, sp_size):
    tokens, dim = x_ref.shape
    layers = w_in_ref.shape[0]
    parts, _, seq, _ = recv_ref.shape[1:]
    me = lax.axis_index('cp') * sp_size + lax.axis_index('sp')
    q_steps = dim // QW
    m_steps = (w_out_ref.shape[1] - dim) // MW
    halves = NDEV // QH
    chips = NDEV // 2
    q_rows = seq // chips
    n_keys = seq // KC
    kinds = 3
    factor = (HEAD ** -0.5) * LOG2E
    vt_ref = wout_ref.at[0, KC:KC + HEAD, :]
    qt_ref = wout_ref.at[1, KC:KC + HEAD, :q_rows]
    even = lax.broadcasted_iota(jnp.int32, (1, HEAD), 1) % 2 == 0
    moved = send_ref.at[pl.ds(0, NDEV - 1)]
    moved_head = send_ref.at[pl.ds(0, NDEV - 1), 0]

    def in_copy(layer, col, slot, idx):
        return pltpu.make_async_copy(w_in_ref.at[layer, :, pl.ds(pl.multiple_of(col, QW), QW)], win_ref.at[slot, idx], in_sem.at[slot, idx])

    def out_copy(layer, step, slot):
        return pltpu.make_async_copy(w_out_ref.at[layer, pl.ds(pl.multiple_of(dim + step * MW, MW), MW), :], wout_ref.at[slot], out_sem.at[slot])

    def attn_w_copy(layer, n):
        return pltpu.make_async_copy(w_out_ref.at[layer, pl.ds(0, dim), pl.ds(n * QW, QW)], win_ref.at[n // kinds, n % kinds], in_sem.at[n // kinds, n % kinds])

    def q_cols(step):
        return [w * dim + step * QW for w in range(kinds)]

    def m_cols(step):
        return [kinds * dim + step * MW + i * QW for i in range(MW // QW)]

    x_in = pltpu.make_async_copy(x_hbm, x_ref, io_sem)
    x_in.start()
    for w, col in enumerate(q_cols(0)):
        in_copy(0, col, 0, w).start()
    barrier = meet_all(me, sp_size)
    mask_at = (NDEV - 1) * (mods_ref.shape[1] // NDEV)
    mask_ref[...] = jnp.broadcast_to(mods_ref[MASK_ROW:MASK_ROW + 1, mask_at:mask_at + tokens], (HEAD, tokens)).T
    x_in.wait()

    for layer in range(layers):

        def q_landing(part, layer=layer):
            return recv_ref.at[layer, part, :, pl.ds(pl.multiple_of(me * tokens, tokens), tokens), :]

        def q_keep(part, layer=layer):
            return pltpu.make_async_copy(send_ref.at[part * NDEV + me], q_landing(part), qk_sem.at[layer, part])

        def q_send(step, layer=layer):
            part = step // halves
            for dd in range(QH):
                dest = (step % halves) * QH + dd

                @pl.when(dest != me)
                def _():
                    pltpu.make_async_remote_copy(
                        src_ref=send_ref.at[part * NDEV + dest], dst_ref=q_landing(part),
                        send_sem=qs_sem.at[layer, part], recv_sem=qr_sem.at[layer, part],
                        device_id=device_of(dest, sp_size), device_id_type=pl.DeviceIdType.MESH).start()

                @pl.when(dest == me)
                def _():
                    q_keep(part).start()

        def q_arrived(part, layer=layer):
            pltpu.make_async_copy(moved, moved, qr_sem.at[layer, part]).wait()
            q_keep(part).wait()

        def q_sent(part, layer=layer):
            pltpu.make_async_copy(moved, moved, qs_sem.at[layer, part]).wait()

        rows = 16
        shift = mods_ref[layer:layer + 1, :dim]
        scale_p = 1.0 + mods_ref[layer:layer + 1, dim:2 * dim]
        bias_out = jnp.broadcast_to(bo_ref[...].astype(jnp.float32)[layer:layer + 1], (rows, dim))
        gains = [g_ref[...].astype(jnp.float32)[layer:layer + 1] for g_ref in (qg_ref, kg_ref)]

        def norm_rows(r, carry):
            at = pl.ds(pl.multiple_of(r * rows, rows), rows)
            v = x_ref[at, :].astype(jnp.float32)
            v = v - jnp.mean(v, axis=-1, keepdims=True)
            var = jnp.mean(v * v, axis=-1, keepdims=True)
            h_ref[at, :] = (v * lax.rsqrt(var + EPS) * scale_p + shift).astype(jnp.bfloat16)
            y_ref[at, :] = bias_out
            return carry

        lax.fori_loop(0, tokens // rows, norm_rows, 0, unroll=4)

        def project(slot, idx, col, layer=layer):
            acc = jnp.dot(h_ref[...], win_ref[slot, idx], preferred_element_type=jnp.float32)
            bias = b_ref[:, pl.ds(pl.multiple_of(col, QW), QW)].astype(jnp.float32)[layer:layer + 1]
            return (acc + bias).astype(jnp.bfloat16)

        def q_step(t, carry, layer=layer):
            slot = t % 2
            for w, col in enumerate(q_cols(t)):
                in_copy(layer, col, slot, w).wait()

            @pl.when(t + 1 < q_steps)
            def _():
                for w, col in enumerate(q_cols(t + 1)):
                    in_copy(layer, col, 1 - slot, w).start()

            @pl.when(t + 1 == q_steps)
            def _():
                for i, col in enumerate(m_cols(0)):
                    in_copy(layer, col, 1 - slot, i).start()
                out_copy(layer, 0, 1 - slot).start()

            if layer == 0:
                @pl.when(t == 1)
                def _():
                    pl.semaphore_wait(barrier, NDEV - 1)

            @pl.when(t > 0)
            def _():
                q_send(t - 1)

            for w, col in enumerate(q_cols(t)):
                u = project(slot, w, col)
                for n in range(QH):
                    piece = u[:, n * HEAD:(n + 1) * HEAD]
                    if w < 2:
                        v = piece.astype(jnp.float32)
                        v = v * lax.rsqrt(jnp.mean(v * v, axis=-1, keepdims=True) + EPS) * gains[w]
                        swapped = jnp.where(even, pltpu.roll(v, HEAD - 1, 1), pltpu.roll(v, 1, 1))
                        piece = (v * cos_ref[...] + swapped * sin_ref[...]).astype(jnp.bfloat16)
                    send_ref[t * QH + n, w] = piece
            return carry

        lax.fori_loop(0, q_steps, q_step, 0)

        def kv_copy(part, slot, layer=layer):
            return pltpu.make_async_copy(recv_ref.at[layer, part], kv_ref.at[slot], kv_sem.at[slot])

        def m_step(b, carry, layer=layer):
            slot = (q_steps + b) % 2
            for i, col in enumerate(m_cols(b)):
                in_copy(layer, col, slot, i).wait()
            out_copy(layer, b, slot).wait()

            @pl.when(b + 1 < m_steps)
            def _():
                for i, col in enumerate(m_cols(b + 1)):
                    in_copy(layer, col, 1 - slot, i).start()
                out_copy(layer, b + 1, 1 - slot).start()

            @pl.when(b == 0)
            def _():
                q_send(q_steps - 1)

            @pl.when(b == m_steps - 1)
            def _():
                q_arrived(0)
                kv_copy(0, 0).start()

            for i, col in enumerate(m_cols(b)):
                v = project(slot, i, col).astype(jnp.float32)
                inner = v * (0.7978845608028654 + (0.7978845608028654 * 0.044715) * (v * v))
                half = 0.5 * v
                act_ref[i] = (half + half * jnp.tanh(inner)).astype(jnp.bfloat16)
            for i in range(MW // QW):
                y_ref[...] += jnp.dot(act_ref[i], wout_ref[slot, i * QW:(i + 1) * QW, :], preferred_element_type=jnp.float32)
            return carry

        lax.fori_loop(0, m_steps, m_step, 0)
        for n in range(q_steps):
            attn_w_copy(layer, n).start()

        def chip_at(t):
            return (me // 2 + 1 + t % chips) % chips

        def a_source(part, dest):
            return send_ref.at[part * NDEV + dest, 0]

        def a_landing(part):
            return a_ref.at[:, pl.ds(pl.multiple_of((part * NDEV + me) * HEAD, HEAD), HEAD)]

        def a_keep(part, layer=layer):
            return pltpu.make_async_copy(a_source(part, me), a_landing(part), ak_sem.at[layer, part])

        def a_send(t, layer=layer):
            part = t // chips
            for core in range(2):
                dest = chip_at(t) * 2 + core

                @pl.when(dest != me)
                def _():
                    pltpu.make_async_remote_copy(
                        src_ref=a_source(part, dest), dst_ref=a_landing(part),
                        send_sem=as_sem.at[layer, part], recv_sem=ar_sem.at[layer, part],
                        device_id=device_of(dest, sp_size), device_id_type=pl.DeviceIdType.MESH).start()

                @pl.when(dest == me)
                def _():
                    a_keep(part).start()

        def a_arrived(part, layer=layer):
            pltpu.make_async_copy(moved_head, moved_head, ar_sem.at[layer, part]).wait()
            a_keep(part).wait()

        def attend(t, carry):
            part = t // chips
            slot = part % 2
            chip = chip_at(t)

            @pl.when(t > 0)
            def _():
                a_send(t - 1)

            @pl.when(t % chips == 0)
            def _():
                q_sent(part)
                kv_copy(part, slot).wait()

                @pl.when(part + 1 < parts)
                def _():
                    q_arrived(part + 1)
                    kv_copy(part + 1, 1 - slot).start()

                for c in range(n_keys):
                    vt_ref[:, c * KC:(c + 1) * KC] = kv_ref[slot, 2, c * KC:(c + 1) * KC, :].T

            qt_ref[...] = kv_ref[slot, 0, pl.ds(pl.multiple_of(chip * q_rows, q_rows), q_rows), :].T
            maxes = [jnp.full((1, q_rows), -1e30, jnp.float32)]

            def scores(c):
                s = jnp.dot(kv_ref[slot, 1, c * KC:(c + 1) * KC, :], qt_ref[...], preferred_element_type=jnp.float32)
                if c + 1 == n_keys:
                    valid = jnp.concatenate([mask_ref[...]] * (q_rows // HEAD), axis=1) > 0
                    s = jnp.concatenate([s[:KC - tokens], jnp.where(valid, s[KC - tokens:], -1e30)], axis=0)
                s_ref[c % 2] = s
                maxes.append(jnp.maximum(maxes[-1], jnp.max(s, axis=0, keepdims=True)))

            total = acc = None
            scores(0)
            for c in range(n_keys):
                if c + 1 < n_keys:
                    scores(c + 1)
                p = jnp.exp2((s_ref[c % 2] - maxes[c + 1]) * factor)
                row = jnp.sum(p, axis=0, keepdims=True)
                wout_ref[c % 2, :KC, :q_rows] = p.astype(jnp.bfloat16)
                pv = jnp.dot(vt_ref[:, c * KC:(c + 1) * KC], wout_ref[c % 2, :KC, :q_rows], preferred_element_type=jnp.float32)
                if c == 0:
                    total, acc = row, pv
                else:
                    alpha = jnp.exp2((maxes[c] - maxes[c + 1]) * factor)
                    total, acc = total * alpha + row, acc * alpha + pv
            out = (acc * (1.0 / total)).astype(jnp.bfloat16).T
            for core in range(2):
                send_ref[part * NDEV + chip * 2 + core, 0] = out[core * tokens:(core + 1) * tokens]
            return carry

        lax.fori_loop(0, parts * chips, attend, 0)
        a_send(parts * chips - 1)

        for n in range(q_steps):
            attn_w_copy(layer, n).wait()
        for part in range(parts - 1):
            a_arrived(part)
        split = (parts - 1) * NDEV * HEAD

        def attn_w(n, cut):
            return win_ref[n // kinds, n % kinds, cut, :]

        for n in range(q_steps):
            cols = slice(n * QW, (n + 1) * QW)
            y_ref[:, cols] += jnp.dot(a_ref[:, :split], attn_w(n, slice(0, split)), preferred_element_type=jnp.float32)
        a_arrived(parts - 1)
        for n in range(q_steps):
            cols = slice(n * QW, (n + 1) * QW)
            y = y_ref[:, cols] + jnp.dot(a_ref[:, split:], attn_w(n, slice(split, dim)), preferred_element_type=jnp.float32)
            gate = mods_ref[layer:layer + 1, 2 * dim + n * QW:2 * dim + (n + 1) * QW]
            x_ref[:, cols] = (x_ref[:, cols].astype(jnp.float32) + gate * y).astype(jnp.bfloat16)
            if n + 1 == kinds and layer + 1 < layers:
                for w, col in enumerate(q_cols(0)):
                    in_copy(layer + 1, col, 0, w).start()
        for part in range(parts):
            pltpu.make_async_copy(moved_head, moved_head, as_sem.at[layer, part]).wait()

    x_out = pltpu.make_async_copy(x_ref, o_hbm, io_sem)
    x_out.start()
    x_out.wait()


def blocks(state, mods, b_in, b_out, q_gain, k_gain, cos_t, sin_t, w_in, w_out, sp_size):
    tokens, dim = state.shape
    layers = w_in.shape[0]
    mlp_dim = w_out.shape[1] - dim
    parts = dim // (NDEV * HEAD)
    seq = NDEV * tokens
    q_rows = seq // (NDEV // 2)
    vmem = pl.BlockSpec(memory_space=pltpu.VMEM)
    hbm = pl.BlockSpec(memory_space=pl.ANY)
    dma = pltpu.SemaphoreType.DMA
    flops = layers * (2 * tokens * dim * (4 * dim + 2 * mlp_dim) + 4 * parts * seq * seq * HEAD)
    out, _ = pl.pallas_call(
        functools.partial(blocks_body, sp_size=sp_size),
        out_shape=(jax.ShapeDtypeStruct((tokens, dim), jnp.bfloat16),
                   jax.ShapeDtypeStruct((layers, parts, 3, seq, HEAD), jnp.bfloat16)),
        in_specs=[hbm] + [vmem] * 7 + [hbm, hbm],
        out_specs=(hbm, hbm),
        scratch_shapes=[
            pltpu.VMEM((tokens, dim), jnp.bfloat16),
            pltpu.VMEM((tokens, dim), jnp.bfloat16),
            pltpu.VMEM((tokens, dim), jnp.float32),
            pltpu.VMEM((2, 3, dim, QW), jnp.bfloat16),
            pltpu.VMEM((2, MW, dim), jnp.bfloat16),
            pltpu.VMEM((parts * NDEV, 3, tokens, HEAD), jnp.bfloat16),
            pltpu.VMEM((MW // QW, tokens, QW), jnp.bfloat16),
            pltpu.VMEM((2, 3, seq, HEAD), jnp.bfloat16),
            pltpu.VMEM((2, KC, q_rows), jnp.float32),
            pltpu.VMEM((tokens, HEAD), jnp.float32),
            pltpu.VMEM((tokens, dim), jnp.bfloat16),
            dma((2, 3)), dma((2,)), dma, dma((2,)),
            dma((layers, parts)), dma((layers, parts)), dma((layers, parts)),
            dma((layers, parts)), dma((layers, parts)), dma((layers, parts)),
        ],
        compiler_params=pltpu.CompilerParams(collective_id=0, has_side_effects=True, vmem_limit_bytes=67043328),
        cost_estimate=pl.CostEstimate(flops=flops, bytes_accessed=2 * layers * dim * (4 * dim + 2 * mlp_dim), transcendentals=layers * parts * seq * seq),
        name='blocks',
    )(state, mods, b_in, b_out, q_gain, k_gain, cos_t, sin_t, w_in, w_out)
    return out


def solution(mesh):
    tok_spec = P('part', AXES, None)
    mask_spec = P('part', AXES)
    vec_spec = P('part', None)
    rep = P()

    def local_blocks(hidden, valid_mask, positions, cond_vec, w_mod, b_mod, w_in, b_in, q_gain, k_gain, w_out, b_out):
        sp_size = mesh.shape['sp']
        mods, cos_t, sin_t = modulation(cond_vec, positions[0].T, valid_mask, b_mod, w_mod, sp_size)
        state = blocks(hidden[0], mods, b_in, b_out, q_gain, k_gain, cos_t, sin_t, w_in, w_out, sp_size)
        return state[None]

    in_specs = (tok_spec, mask_spec, tok_spec, vec_spec, rep, rep, rep, rep, rep, rep, rep, rep)
    return jax.shard_map(local_blocks, mesh=mesh, in_specs=in_specs, out_specs=tok_spec, check_vma=False)
```
